16 devices in a mesh: rep: 4 (over y, z, core), dp: 4 (over x).
Axes of the slice: x: 4, y: 2, z: 1, core: 2. Of those that a mesh axis runs over, the one named last changes fastest.
The devices are a block of a 4x4x8 slice.
Arguments:
- x: bfloat16 [16, 4096, 640], P(('rep', 'dp')), parts along dimension 0
- dy: bfloat16 [16, 4096, 640], P(('rep', 'dp')), parts along dimension 0
- w_gate: bfloat16 [2, 640, 2048], replicated
- w_up: bfloat16 [2, 640, 2048], replicated
- w_down: bfloat16 [2, 2048, 640], replicated
- m_w_gate: float32 [2, 640, 2048], P(None, 'dp')
- m_w_up: float32 [2, 640, 2048], P(None, 'dp')
- m_w_down: float32 [2, 2048, 640], P(None, 'dp')
- v_w_gate: float32 [2, 640, 2048], P(None, 'dp')
- v_w_up: float32 [2, 640, 2048], P(None, 'dp')
- v_w_down: float32 [2, 2048, 640], P(None, 'dp')
Outputs:
- output 1: bfloat16 [8, 640, 2048], P('rep'), parts along dimension 0
- output 2: bfloat16 [8, 640, 2048], P('rep'), parts along dimension 0
- output 3: bfloat16 [8, 2048, 640], P('rep'), parts along dimension 0
- output 4: float32 [8, 640, 2048], P('rep', 'dp'), parts along dimension 0
- output 5: float32 [8, 640, 2048], P('rep', 'dp'), parts along dimension 0
- output 6: float32 [8, 2048, 640], P('rep', 'dp'), parts along dimension 0
- output 7: float32 [8, 640, 2048], P('rep', 'dp'), parts along dimension 0
- output 8: float32 [8, 640, 2048], P('rep', 'dp'), parts along dimension 0
- output 9: float32 [8, 2048, 640], P('rep', 'dp'), parts along dimension 0
There are 4 independent parts. The reference program is written for one: setup_inputs(seed, part) draws one part's arguments, and reference() takes and returns one part's arrays. A program takes and returns all parts, laid end to end along the dimension named above; an argument that names none is the same for every part.
All inputs are finite; a program needn't handle non-finite values.
Results may differ from the reference program's by a relative error of at most 0.022.
Values are sent between devices in bfloat16 or wider.
A program may use at most 768 MiB of HBM per device.

```python
import jax
import jax.numpy as jnp
from jax import lax

SEQUENCES = 4
TOKENS = 4096
D = 640
FF = 2048
LAYERS = 2
NAMES = ("w_gate", "w_up", "w_down")
SHAPES = {"w_gate": (LAYERS, D, FF), "w_up": (LAYERS, D, FF), "w_down": (LAYERS, FF, D)}


def bump(key, n, height):
    away = (jnp.arange(n, dtype=jnp.int32) - jax.random.randint(key, (), 0, n, jnp.int32)) % n
    return jnp.where(away < n // 8, height, 1.0)


def together(key, own, strength):
    shared = jax.random.normal(key, own.shape[1:], jnp.float32)
    return (own + strength * shared) * lax.rsqrt(1 + strength * strength)


def setup_inputs(seed: int = 0, part: int = 0) -> dict:
    kx, kdy, ka, kb, kz, kf, kh, kl, *keys = jax.random.split(jax.random.key(seed), 8 + 3 * len(NAMES))
    kx, kdy, ka, kb = (jax.random.fold_in(k, part) for k in (kx, kdy, ka, kb))
    kw, km, kv = (keys[i::3] for i in range(3))
    shape = (SEQUENCES, TOKENS, D)
    much_x, much_dy = jax.random.uniform(kz, (2,), jnp.float32, 0.0, 1.0)
    loud = 2.0 ** jax.random.uniform(jax.random.fold_in(kz, 1), (), jnp.float32, -1.0, 2.0)
    layers = 2.0 ** jax.random.uniform(kl, (LAYERS, 1, 1), jnp.float32, -1.0, 1.0)
    x = together(ka, jax.random.normal(kx, shape, jnp.float32), much_x) * bump(kf, D, 4.0)
    dy = together(kb, jax.random.normal(kdy, shape, jnp.float32), much_dy)
    drawn = {"x": x.astype(jnp.bfloat16), "dy": (loud * dy * (SEQUENCES * TOKENS) ** -0.5).astype(jnp.bfloat16)}
    for key, name in zip(kw, NAMES, strict=True):
        w = jax.random.normal(key, SHAPES[name], jnp.float32) * SHAPES[name][1] ** -0.5
        drawn[name] = (w * {"w_gate": 1.0, "w_up": bump(kh, FF, 4.0), "w_down": layers}[name]).astype(jnp.bfloat16)
    for key, name in zip(km, NAMES, strict=True):
        drawn[f"m_{name}"] = 0.1 * jax.random.normal(key, SHAPES[name], jnp.float32)
    for key, name in zip(kv, NAMES, strict=True):
        drawn[f"v_{name}"] = jax.random.uniform(key, SHAPES[name], jnp.float32, 0.005, 0.015)
    return drawn


def matmul(a, w):
    return jnp.dot(a, w, preferred_element_type=jnp.float32).astype(jnp.bfloat16)


def normed(h):
    wide = h.astype(jnp.float32)
    scale = lax.rsqrt(jnp.mean(wide**2, -1, keepdims=True) + 1e-6)
    return (wide * scale).astype(jnp.bfloat16)


def layer(h, w):
    a = normed(h)
    gate = jnp.dot(a, w["w_gate"], preferred_element_type=jnp.float32)
    up = jnp.dot(a, w["w_up"], preferred_element_type=jnp.float32)
    return h + matmul((jax.nn.silu(gate) * up).astype(jnp.bfloat16), w["w_down"])


def adamw(w, m, v, g):
    m = 0.9 * m + 0.1 * g
    v = 0.95 * v + 0.05 * g * g
    step = m * lax.rsqrt(v + 1e-8) + 0.1 * w
    return (w - 0.02 * step).astype(jnp.bfloat16), m, v


def clipped(gradients, sum_of_squares, count):
    factor = jnp.minimum(1.0, 0.5 * lax.rsqrt(sum_of_squares / count + 1e-30))
    return [g * factor for g in gradients]


def stack(weights, h):
    return lax.scan(lambda h, w: (layer(h, w), None), h, weights)[0]


def reference(x, dy, w_gate, w_up, w_down, m_w_gate, m_w_up, m_w_down, v_w_gate, v_w_up, v_w_down):
    weights = dict(zip(NAMES, (w_gate, w_up, w_down), strict=True))

    def take(so_far, sequence):
        h, by_y = sequence
        _, back = jax.vjp(lambda w: stack(w, h), weights)
        return jax.tree.map(lambda total, term: total + term.astype(jnp.float32), so_far, back(by_y)[0]), None

    none_yet = {name: jnp.zeros(w.shape, jnp.float32) for name, w in weights.items()}
    by_weights, _ = lax.scan(take, none_yet, (x, dy))
    gradients = [by_weights[name].astype(jnp.bfloat16).astype(jnp.float32) for name in NAMES]
    gradients = clipped(gradients, sum(jnp.sum(g * g) for g in gradients), sum(g.size for g in gradients))
    new = [
        adamw(w.astype(jnp.float32), m, v, g)
        for w, m, v, g in zip((w_gate, w_up, w_down), (m_w_gate, m_w_up, m_w_down), (v_w_gate, v_w_up, v_w_down), gradients, strict=True)
    ]
    return tuple(one[which] for which in range(3) for one in new)
```

```python
import functools

import jax
import jax.numpy as jnp
from jax import lax
from jax.experimental import pallas as pl
from jax.experimental.pallas import tpu as pltpu
from jax.sharding import PartitionSpec as P

F32, BF16 = jnp.float32, jnp.bfloat16
VMEM_BYTES = 66_000_000
NN = (((1,), (0,)), ((), ()))
NT = (((1,), (1,)), ((), ()))
TN = (((0,), (0,)), ((), ()))


def dot(a, b, dims=NN):
    return lax.dot_general(a, b, dims, preferred_element_type=F32)


def params(**more):
    return pltpu.CompilerParams(vmem_limit_bytes=VMEM_BYTES, **more)


def cost(flops, nbytes):
    return pl.CostEstimate(flops=flops, bytes_accessed=nbytes, transcendentals=0)


def tokens_spec(tile, width):
    return pl.BlockSpec((tile, width), lambda i: (i, 0))


def weight_spec(w, layer):
    return pl.BlockSpec((None, *w.shape[1:]), lambda i: (layer, 0, 0), pipeline_mode=pl.Buffered(1))


def scale_of(wide):
    return lax.rsqrt(jnp.mean(wide * wide, -1, keepdims=True) + 1e-6)


def gated(gate, up):
    sig = 0.5 * jnp.tanh(0.5 * gate) + 0.5
    act = gate * sig
    return act, up * (sig + act * (1.0 - sig)), (act * up).astype(BF16)


def first_kernel(chunk, x_ref, wg, wu, wd, act_ref, slope_ref, hid_ref, h1_ref, a_ref):
    wide = x_ref[...].astype(F32)
    a = (wide * scale_of(wide)).astype(BF16)
    a_ref[...] = a
    for c in range(0, wg.shape[1], chunk):
        at = pl.ds(c, chunk)
        act, slope, hid = gated(dot(a, wg[:, at]), dot(a, wu[:, at]))
        act_ref[:, at] = act
        slope_ref[:, at] = slope
        hid_ref[:, at] = hid
    y = dot(hid_ref[...], wd[...]).astype(BF16)
    h1_ref[...] = (wide + y.astype(F32)).astype(BF16)


def first(x, wg, wu, wd, tile=512, chunk=512):
    t, d = x.shape
    f = wg.shape[2]
    return pl.pallas_call(
        functools.partial(first_kernel, chunk),
        grid=(t // tile,),
        in_specs=[tokens_spec(tile, d), weight_spec(wg, 0), weight_spec(wu, 0), weight_spec(wd, 0)],
        out_specs=[tokens_spec(tile, f)] * 3 + [tokens_spec(tile, d)] * 2,
        out_shape=[
            jax.ShapeDtypeStruct((t, f), F32),
            jax.ShapeDtypeStruct((t, f), F32),
            jax.ShapeDtypeStruct((t, f), BF16),
            jax.ShapeDtypeStruct((t, d), BF16),
            jax.ShapeDtypeStruct((t, d), BF16),
        ],
        compiler_params=params(),
        cost_estimate=cost(6 * t * d * f, 10 * t * f),
        name="first",
    )(x, wg, wu, wd)


def second_kernel(chunk, h_ref, dy_ref, wg, wu, wd, hid_ref, dgate_ref, dup_ref, a_ref):
    wide = h_ref[...].astype(F32)
    a = (wide * scale_of(wide)).astype(BF16)
    a_ref[...] = a
    dy = dy_ref[...]
    for c in range(0, wg.shape[1], chunk):
        at = pl.ds(c, chunk)
        act, slope, hid = gated(dot(a, wg[:, at]), dot(a, wu[:, at]))
        hid_ref[:, at] = hid
        dhid = dot(dy, wd[at, :], NT).astype(BF16).astype(F32)
        dgate_ref[:, at] = (dhid * slope).astype(BF16)
        dup_ref[:, at] = (dhid * act).astype(BF16)


def second(h, dy, wg, wu, wd, tile=512, chunk=512):
    t, d = h.shape
    f = wg.shape[2]
    return pl.pallas_call(
        functools.partial(second_kernel, chunk),
        grid=(t // tile,),
        in_specs=[tokens_spec(tile, d)] * 2 + [weight_spec(wg, 1), weight_spec(wu, 1), weight_spec(wd, 1)],
        out_specs=[tokens_spec(tile, f)] * 3 + [tokens_spec(tile, d)],
        out_shape=[jax.ShapeDtypeStruct((t, f), BF16)] * 3 + [jax.ShapeDtypeStruct((t, d), BF16)],
        compiler_params=params(),
        cost_estimate=cost(6 * t * d * f, 6 * t * f),
        name="second",
    )(h, dy, wg, wu, wd)


def third_kernel(chunk, dgate_ref, dup_ref, h_ref, dy_ref, act_ref, slope_ref, wg, wu, wd, dh_ref, dgate0_ref, dup0_ref):
    da = dot(dgate_ref[...], wg[...], NT).astype(BF16) + dot(dup_ref[...], wu[...], NT).astype(BF16)
    da = da.astype(F32)
    wide = h_ref[...].astype(F32)
    scale = scale_of(wide)
    along = jnp.mean(da * wide, -1, keepdims=True)
    dn = da * scale - wide * (scale * scale * scale * along)
    dh = (dy_ref[...].astype(F32) + dn.astype(BF16).astype(F32)).astype(BF16)
    dh_ref[...] = dh
    for c in range(0, wd.shape[0], chunk):
        at = pl.ds(c, chunk)
        dhid = dot(dh, wd[at, :], NT).astype(BF16).astype(F32)
        dgate0_ref[:, at] = (dhid * slope_ref[:, at]).astype(BF16)
        dup0_ref[:, at] = (dhid * act_ref[:, at]).astype(BF16)


def third(dgate, dup, h, dy, act, slope, wg, wu, wd, tile=512, chunk=512):
    t, d = h.shape
    f = wg.shape[2]
    return pl.pallas_call(
        functools.partial(third_kernel, chunk),
        grid=(t // tile,),
        in_specs=[tokens_spec(tile, f)] * 2
        + [tokens_spec(tile, d)] * 2
        + [tokens_spec(tile, f)] * 2
        + [weight_spec(wg, 1), weight_spec(wu, 1), weight_spec(wd, 0)],
        out_specs=[tokens_spec(tile, d)] + [tokens_spec(tile, f)] * 2,
        out_shape=[jax.ShapeDtypeStruct((t, d), BF16)] + [jax.ShapeDtypeStruct((t, f), BF16)] * 2,
        compiler_params=params(),
        cost_estimate=cost(6 * t * d * f, 16 * t * f),
        name="third",
    )(dgate, dup, h, dy, act, slope, wg, wu, wd)


def outer_kernel(flip, a_ref, b_ref, o_ref):
    out = dot(a_ref[...], b_ref[...], TN)
    o_ref[...] = (out.T if flip else out).astype(BF16)


def outer(a, b, flip, name, tile=512):
    t, d = a.shape
    f = b.shape[1]
    return pl.pallas_call(
        functools.partial(outer_kernel, flip),
        grid=(f // tile,),
        in_specs=[
            pl.BlockSpec((t, d), lambda i: (0, 0), pipeline_mode=pl.Buffered(1)),
            pl.BlockSpec((t, tile), lambda i: (0, i)),
        ],
        out_specs=pl.BlockSpec((tile, d), lambda i: (i, 0)) if flip else pl.BlockSpec((d, tile), lambda i: (0, i)),
        out_shape=jax.ShapeDtypeStruct((f, d) if flip else (d, f), BF16),
        compiler_params=params(),
        cost_estimate=cost(2 * t * d * f, 2 * t * f),
        name=name,
    )(a, b)


def adamw(w, m, v, g):
    m = 0.9 * m + 0.1 * g
    v = 0.95 * v + 0.05 * g * g
    step = m * lax.rsqrt(v + 1e-8) + 0.1 * w
    return (w - 0.02 * step).astype(BF16), m, v


def solution(mesh):
    def scatter(dw):
        return lax.psum_scatter(dw, "dp", scatter_dimension=0, tiled=True)

    def body(x, dy, wg, wu, wd, *moments):
        m, v = moments[:3], moments[3:]
        x, dy = x[0], dy[0]
        act0, slope0, hid0, h1, a0 = first(x, wg, wu, wd)
        hid1, dgate1, dup1, a1 = second(h1, dy, wg, wu, wd)
        gd1 = scatter(outer(dy, hid1, True, "dwd1"))
        gg1 = scatter(outer(a1, dgate1, False, "dwg1"))
        gu1 = scatter(outer(a1, dup1, False, "dwu1"))
        dh1, dgate0, dup0 = third(dgate1, dup1, h1, dy, act0, slope0, wg, wu, wd)
        gd0 = scatter(outer(dh1, hid0, True, "dwd0"))
        gg0 = scatter(outer(a0, dgate0, False, "dwg0"))
        gu0 = scatter(outer(a0, dup0, False, "dwu0"))
        grads = [[t.astype(F32) for t in pair] for pair in ((gg0, gg1), (gu0, gu1), (gd0, gd1))]
        total = lax.psum(sum(jnp.sum(g * g) for pair in grads for g in pair), "dp")
        count = sum(w.size for w in (wg, wu, wd))
        factor = jnp.minimum(1.0, 0.5 * lax.rsqrt(total / count + 1e-30))
        me = lax.axis_index("dp")
        new = []
        for w, mw, vw, pair in zip((wg, wu, wd), m, v, grads, strict=True):
            g = jnp.stack(pair) * factor
            rows = mw.shape[1]
            mine = lax.dynamic_slice_in_dim(w, me * rows, rows, 1).astype(F32)
            nw, nm, nv = adamw(mine, mw, vw, g)
            new.append((lax.all_gather(nw, "dp", axis=1, tiled=True), nm, nv))
        return tuple(one[which] for which in range(3) for one in new)

    whole, rows = P(None, None, None), P(None, "dp", None)
    return jax.shard_map(
        body,
        mesh=mesh,
        in_specs=(P(("rep", "dp")),) * 2 + (whole,) * 3 + (rows,) * 6,
        out_specs=(P("rep"),) * 3 + (P("rep", "dp"),) * 6,
        check_vma=False,
    )
```

```python
import functools

import jax
import jax.numpy as jnp
from jax import lax
from jax.experimental import pallas as pl
from jax.experimental.pallas import tpu as pltpu
from jax.sharding import PartitionSpec as P

F32, BF16 = jnp.float32, jnp.bfloat16
VMEM_BYTES = 66_000_000
NN = (((1,), (0,)), ((), ()))
NT = (((1,), (1,)), ((), ()))
TN = (((0,), (0,)), ((), ()))


def dot(a, b, dims=NN):
    return lax.dot_general(a, b, dims, preferred_element_type=F32)


def params(**more):
    return pltpu.CompilerParams(vmem_limit_bytes=VMEM_BYTES, **more)


def cost(flops, nbytes):
    return pl.CostEstimate(flops=flops, bytes_accessed=nbytes, transcendentals=0)


def tokens_spec(tile, width):
    return pl.BlockSpec((tile, width), lambda i: (i, 0))


def weight_spec(w, layer):
    return pl.BlockSpec((None, *w.shape[1:]), lambda i: (layer, 0, 0), pipeline_mode=pl.Buffered(1))


def scale_of(wide):
    return lax.rsqrt(jnp.mean(wide * wide, -1, keepdims=True) + 1e-6)


def gated(gate, up):
    sig = 0.5 * jnp.tanh(0.5 * gate) + 0.5
    act = gate * sig
    return act, up * (sig + act * (1.0 - sig)), (act * up).astype(BF16)


def first_kernel(chunk, x_ref, wg, wu, wd, act_ref, slope_ref, hid_ref, h1_ref, a_ref):
    wide = x_ref[...].astype(F32)
    a = (wide * scale_of(wide)).astype(BF16)
    a_ref[...] = a
    for c in range(0, wg.shape[1], chunk):
        at = pl.ds(c, chunk)
        act, slope, hid = gated(dot(a, wg[:, at]), dot(a, wu[:, at]))
        act_ref[:, at] = act
        slope_ref[:, at] = slope
        hid_ref[:, at] = hid
    y = dot(hid_ref[...], wd[...]).astype(BF16)
    h1_ref[...] = (wide + y.astype(F32)).astype(BF16)


def first(x, wg, wu, wd, tile=512, chunk=512):
    t, d = x.shape
    f = wg.shape[2]
    return pl.pallas_call(
        functools.partial(first_kernel, chunk),
        grid=(t // tile,),
        in_specs=[tokens_spec(tile, d), weight_spec(wg, 0), weight_spec(wu, 0), weight_spec(wd, 0)],
        out_specs=[tokens_spec(tile, f)] * 3 + [tokens_spec(tile, d)] * 2,
        out_shape=[
            jax.ShapeDtypeStruct((t, f), F32),
            jax.ShapeDtypeStruct((t, f), F32),
            jax.ShapeDtypeStruct((t, f), BF16),
            jax.ShapeDtypeStruct((t, d), BF16),
            jax.ShapeDtypeStruct((t, d), BF16),
        ],
        compiler_params=params(),
        cost_estimate=cost(6 * t * d * f, 10 * t * f),
        name="first",
    )(x, wg, wu, wd)


def second_kernel(chunk, h_ref, dy_ref, wg, wu, wd, hid_ref, dgate_ref, dup_ref, a_ref):
    wide = h_ref[...].astype(F32)
    a = (wide * scale_of(wide)).astype(BF16)
    a_ref[...] = a
    dy = dy_ref[...]
    for c in range(0, wg.shape[1], chunk):
        at = pl.ds(c, chunk)
        act, slope, hid = gated(dot(a, wg[:, at]), dot(a, wu[:, at]))
        hid_ref[:, at] = hid
        dhid = dot(dy, wd[at, :], NT).astype(BF16).astype(F32)
        dgate_ref[:, at] = (dhid * slope).astype(BF16)
        dup_ref[:, at] = (dhid * act).astype(BF16)


def second(h, dy, wg, wu, wd, tile=512, chunk=512):
    t, d = h.shape
    f = wg.shape[2]
    return pl.pallas_call(
        functools.partial(second_kernel, chunk),
        grid=(t // tile,),
        in_specs=[tokens_spec(tile, d)] * 2 + [weight_spec(wg, 1), weight_spec(wu, 1), weight_spec(wd, 1)],
        out_specs=[tokens_spec(tile, f)] * 3 + [tokens_spec(tile, d)],
        out_shape=[jax.ShapeDtypeStruct((t, f), BF16)] * 3 + [jax.ShapeDtypeStruct((t, d), BF16)],
        compiler_params=params(),
        cost_estimate=cost(6 * t * d * f, 6 * t * f),
        name="second",
    )(h, dy, wg, wu, wd)


def third_kernel(chunk, dgate_ref, dup_ref, h_ref, dy_ref, act_ref, slope_ref, wg, wu, wd, dh_ref, dgate0_ref, dup0_ref):
    da = dot(dgate_ref[...], wg[...], NT).astype(BF16) + dot(dup_ref[...], wu[...], NT).astype(BF16)
    da = da.astype(F32)
    wide = h_ref[...].astype(F32)
    scale = scale_of(wide)
    along = jnp.mean(da * wide, -1, keepdims=True)
    dn = da * scale - wide * (scale * scale * scale * along)
    dh = (dy_ref[...].astype(F32) + dn.astype(BF16).astype(F32)).astype(BF16)
    dh_ref[...] = dh
    for c in range(0, wd.shape[0], chunk):
        at = pl.ds(c, chunk)
        dhid = dot(dh, wd[at, :], NT).astype(BF16).astype(F32)
        dgate0_ref[:, at] = (dhid * slope_ref[:, at]).astype(BF16)
        dup0_ref[:, at] = (dhid * act_ref[:, at]).astype(BF16)


def third(dgate, dup, h, dy, act, slope, wg, wu, wd, tile=512, chunk=512):
    t, d = h.shape
    f = wg.shape[2]
    return pl.pallas_call(
        functools.partial(third_kernel, chunk),
        grid=(t // tile,),
        in_specs=[tokens_spec(tile, f)] * 2
        + [tokens_spec(tile, d)] * 2
        + [tokens_spec(tile, f)] * 2
        + [weight_spec(wg, 1), weight_spec(wu, 1), weight_spec(wd, 0)],
        out_specs=[tokens_spec(tile, d)] + [tokens_spec(tile, f)] * 2,
        out_shape=[jax.ShapeDtypeStruct((t, d), BF16)] + [jax.ShapeDtypeStruct((t, f), BF16)] * 2,
        compiler_params=params(),
        cost_estimate=cost(6 * t * d * f, 16 * t * f),
        name="third",
    )(dgate, dup, h, dy, act, slope, wg, wu, wd)


def reduce_kernel(flips, axis, tile, steps, last, a_of, *refs):
    n_a = max(a_of) + 1
    a_refs, b_refs, refs = refs[:n_a], refs[n_a : n_a + 3], refs[n_a + 3 :]
    before_ref, g_refs, total_ref, refs = refs[0], refs[1:4], refs[4], refs[5:]
    a_buf, b_buf, wide, flat, a_sem, b_sem, got_all, all_sems, send_sems, recv_sems = refs
    n = 4
    me = lax.axis_index(axis)
    right, left, across = ((me + k) % n for k in (1, 3, 2))

    part = tile // n
    count = 3 * steps

    def load_a(k):
        return pltpu.make_async_copy(a_refs[k], a_buf.at[k], a_sem.at[k])

    def load_b(k, j, slot):
        stride = b_refs[k].shape[1] // n if flips[k] else part
        first = j * part if flips[k] else j * tile
        return [
            pltpu.make_async_copy(
                b_refs[k].at[:, pl.ds(pl.multiple_of(first + q * stride, part), part)],
                b_buf.at[slot, :, pl.ds(q * part, part)],
                b_sem.at[slot, q],
            )
            for q in range(n)
        ]

    load_a(0).start()
    for one in load_b(0, 0, 0):
        one.start()
    for k in range(1, n_a):
        load_a(k).start()

    barrier = pltpu.get_barrier_semaphore()
    peers = (right, left, across) if last else (right, left)
    for peer in peers:
        pl.semaphore_signal(barrier, inc=1, device_id={axis: peer}, device_id_type=pl.DeviceIdType.MESH)

    def sends(kind, s, at, wanted=range(6)):
        full, half = (part, part // 2) if kind else (wide[0].shape[1] // n, wide[0].shape[1] // n // 2)
        out_a, out_r, out_l, in1_l, in1_r, in2_l, in2_r = flat[kind]
        low, high = pl.ds(0, half), pl.ds(half, full - half)
        plan = (
            (out_a, low, in1_l, low, right),
            (out_a, high, in1_r, low, left),
            (out_r, high, in2_l, high, right),
            (out_l, low, in2_r, low, left),
            (out_r, low, in2_l, low, right),
            (out_l, high, in2_r, high, left),
        )
        return {
            which: pltpu.make_async_remote_copy(
                src_ref=src.at[at, rows],
                dst_ref=dst.at[at, to],
                send_sem=send_sems.at[which, s],
                recv_sem=recv_sems.at[which, s],
                device_id={axis: peer},
                device_id_type=pl.DeviceIdType.MESH,
            )
            for which, (src, rows, dst, to, peer) in enumerate(plan)
            if which in wanted
        }

    def rows_of(kind, at, device, start, size):
        full = wide[kind].shape[1] // n
        return wide[kind][at, pl.ds(pl.multiple_of(device * full + start, 16), size), :]

    def half_of(kind):
        return wide[kind].shape[1] // n // 2

    def pass_on(kind, s, at):
        half = half_of(kind)
        out_a, out_r, out_l, in1_l, in1_r, in2_l, in2_r = flat[kind]
        copies = sends(kind, s, at, (0, 1, 4, 5))
        copies[0].wait_recv()
        out_r[at, pl.ds(0, half), :] = (rows_of(kind, at, right, 0, half) + in1_l[at].astype(F32)).astype(BF16)
        copies[4].start()
        copies[1].wait_recv()
        out_l[at, pl.ds(half, half), :] = (rows_of(kind, at, left, half, half) + in1_r[at].astype(F32)).astype(BF16)
        copies[5].start()

    def finish(kind, k, s, j, at):
        full = 2 * half_of(kind)
        in2_l, in2_r = flat[kind][5:]
        copies = sends(kind, s, at, (2, 3, 4, 5))
        for which in (2, 3, 4, 5):
            copies[which].wait_recv()
        g = rows_of(kind, at, me, 0, full) + in2_l[at].astype(F32) + in2_r[at].astype(F32)
        g = g.astype(BF16)
        if kind:
            g_refs[k][pl.ds(pl.multiple_of(j * full, full), full), :] = g
        else:
            g_refs[k][:, pl.ds(pl.multiple_of(j * tile, tile), tile)] = g
        square = g.astype(F32) * g.astype(F32)
        square = jnp.sum(square.reshape(-1, 8, square.shape[1]), 0)
        total_ref[...] += sum(square[:, c : c + 128] for c in range(0, square.shape[1], 128))

    total_ref[...] = before_ref[...]

    base = {}
    seen = [0, 0]
    for k in range(3):
        base[k] = seen[flips[k]]
        seen[flips[k]] += steps

    for k in range(3):
        kind = int(flips[k])
        if k == 0:
            load_a(0).wait()
        elif a_of[k] != a_of[k - 1]:
            load_a(a_of[k]).wait()

        def step(j, _, k=k, kind=kind):
            s = k * steps + j
            at = base[k] + j
            slot = s % 2
            for one in load_b(k, j, slot):
                one.wait()

            @pl.when(j < steps - 1)
            def _():
                for one in load_b(k, j + 1, 1 - slot):
                    one.start()

            if k < 2:

                @pl.when(j == steps - 1)
                def _():
                    for one in load_b(k + 1, 0, 1 - slot):
                        one.start()

            out = dot(a_buf[a_of[k]], b_buf[slot], TN)
            wide[kind][at] = out.T if kind else out
            half = half_of(kind)
            out_a, out_r, out_l = flat[kind][:3]
            out_a[at] = rows_of(kind, at, across, 0, 2 * half).astype(BF16)
            out_r[at, pl.ds(half, half), :] = rows_of(kind, at, right, half, half).astype(BF16)
            out_l[at, pl.ds(0, half), :] = rows_of(kind, at, left, 0, half).astype(BF16)
            if k == 0:

                @pl.when(j == 0)
                def _():
                    pl.semaphore_wait(barrier, len(peers))

            for one in sends(kind, s, at, range(4)).values():
                one.start()

            @pl.when(j > 0)
            def _():
                pass_on(kind, s - 1, at - 1)

            if k > 0:

                @pl.when(j == 0)
                def _():
                    pass_on(int(flips[k - 1]), s - 1, base[k - 1] + steps - 1)

            @pl.when(j > 1)
            def _():
                finish(kind, k, s - 2, j - 2, at - 2)

            if k > 0:

                @pl.when(j < 2)
                def _():
                    finish(int(flips[k - 1]), k - 1, s - 2, j + steps - 2, base[k - 1] + steps - 2 + j)

            return 0

        lax.fori_loop(0, steps, step, 0)

    kind = int(flips[2])
    end = base[2] + steps
    pass_on(kind, count - 1, end - 1)
    finish(kind, 2, count - 2, steps - 2, end - 2)
    finish(kind, 2, count - 1, steps - 1, end - 1)

    for k in range(3):

        def drain(j, _, k=k):
            for one in sends(int(flips[k]), k * steps + j, base[k] + j).values():
                one.wait_send()
            return 0

        lax.fori_loop(0, steps, drain, 0)

    if last:
        got_all[3] = total_ref[...]
        copies = [
            pltpu.make_async_remote_copy(
                src_ref=got_all.at[3],
                dst_ref=got_all.at[to],
                send_sem=all_sems.at[0, to],
                recv_sem=all_sems.at[1, to],
                device_id={axis: peer},
                device_id_type=pl.DeviceIdType.MESH,
            )
            for to, peer in enumerate(peers)
        ]
        for one in copies:
            one.start()
        for one in copies:
            one.wait()
        total_ref[...] = (got_all[0] + got_all[1]) + (got_all[2] + got_all[3])


def reduced(a_list, a_of, b_list, flips, before, last, collective_id, name, tile=512):
    t, d = a_list[0].shape
    f = b_list[0].shape[1]
    steps = f // tile
    n = 4
    shapes = [(d, tile), (tile, d)]
    counts = [steps * (3 - sum(flips)), steps * sum(flips)]

    def buffers(kind):
        rows, columns = shapes[kind]
        full, half = rows // n, rows // n // 2
        return [pltpu.VMEM((counts[kind], r, columns), BF16) for r in (full, full, full, half, half, full, full)]

    any_spec, vmem_spec = pl.BlockSpec(memory_space=pl.ANY), pl.BlockSpec(memory_space=pltpu.VMEM)
    out = [jax.ShapeDtypeStruct((f // n, d) if flip else (d // n, f), BF16) for flip in flips]
    return pl.pallas_call(
        functools.partial(reduce_kernel, flips, "dp", tile, steps, last, a_of),
        in_specs=[any_spec] * (len(a_list) + 3) + [vmem_spec],
        out_specs=[vmem_spec] * 4,
        out_shape=out + [jax.ShapeDtypeStruct((8, 128), F32)],
        scratch_shapes=[
            pltpu.VMEM((len(a_list), t, d), BF16),
            pltpu.VMEM((2, t, tile), BF16),
            [pltpu.VMEM((counts[kind], *shapes[kind]), F32) for kind in range(2)],
            [buffers(kind) for kind in range(2)],
            pltpu.SemaphoreType.DMA((len(a_list),)),
            pltpu.SemaphoreType.DMA((2, n)),
            pltpu.VMEM((4, 8, 128), F32),
            pltpu.SemaphoreType.DMA((2, 3)),
            pltpu.SemaphoreType.DMA((6, 3 * steps)),
            pltpu.SemaphoreType.DMA((6, 3 * steps)),
        ],
        compiler_params=params(collective_id=collective_id, has_side_effects=True),
        cost_estimate=cost(6 * t * d * f, 6 * t * f),
        name=name,
    )(*a_list, *b_list, before)


def adamw(w, m, v, g):
    m = 0.9 * m + 0.1 * g
    v = 0.95 * v + 0.05 * g * g
    step = m * lax.rsqrt(v + 1e-8) + 0.1 * w
    return (w - 0.02 * step).astype(BF16), m, v


def place_kernel(axis, where, *refs):
    blocks, refs = refs[: len(where)], refs[len(where) :]
    outs, sems = refs[-4:-1], refs[-1]
    me = lax.axis_index(axis)
    copies = []
    for k, (matrix, layer, shift, start) in enumerate(where):
        rows = outs[matrix].shape[1] // 4
        at = ((me + shift) % 4) * rows + start
        size = blocks[k].shape[0]
        copies.append(pltpu.make_async_copy(blocks[k], outs[matrix].at[layer, pl.ds(pl.multiple_of(at, 16), size), :], sems.at[k]))
    for one in copies:
        one.start()
    for one in copies:
        one.wait()


def place(blocks, where, shapes, into, name):
    any_spec, vmem_spec = pl.BlockSpec(memory_space=pl.ANY), pl.BlockSpec(memory_space=pltpu.VMEM)
    into = list(into)
    return pl.pallas_call(
        functools.partial(place_kernel, "dp", where),
        in_specs=[vmem_spec] * len(blocks) + [any_spec] * len(into),
        out_specs=[any_spec] * 3,
        out_shape=[jax.ShapeDtypeStruct(s, BF16) for s in shapes],
        scratch_shapes=[pltpu.SemaphoreType.DMA((len(blocks),))],
        input_output_aliases={len(blocks) + k: k for k in range(len(into))},
        compiler_params=params(),
        cost_estimate=cost(1000, sum(b.size for b in blocks) * 4),
        name=name,
    )(*blocks, *into)


def solution(mesh):
    n = mesh.shape["dp"]
    to_right = [(i, (i + 1) % n) for i in range(n)]
    to_left = [(i, (i - 1) % n) for i in range(n)]

    def body(x, dy, wg, wu, wd, *moments):
        m, v = moments[:3], moments[3:]
        x, dy = x[0], dy[0]
        act0, slope0, hid0, h1, a0 = first(x, wg, wu, wd)
        hid1, dgate1, dup1, a1 = second(h1, dy, wg, wu, wd)
        order = (True, False, False)
        gd1, gg1, gu1, total = reduced([dy, a1], (0, 1, 1), [hid1, dgate1, dup1], order, jnp.zeros((8, 128), F32), False, 1, "sum1")
        dh1, dgate0, dup0 = third(dgate1, dup1, h1, dy, act0, slope0, wg, wu, wd)
        gd0, gg0, gu0, total = reduced([dh1, a0], (0, 1, 1), [hid0, dgate0, dup0], order, total, True, 2, "sum0")
        count = sum(w.size for w in (wg, wu, wd))
        factor = jnp.minimum(1.0, 0.5 * lax.rsqrt(jnp.sum(total) / count + 1e-30))
        me = lax.axis_index("dp")
        grads = ((gg0, gg1), (gu0, gu1), (gd0, gd1))
        weights = (wg, wu, wd)
        new_m, new_v, blocks, where = [], [], [], []
        direct = {}
        for k in (0, 1, 2):
            rows = m[k].shape[1]
            made = []
            for layer in range(2):
                mine = lax.dynamic_slice(weights[k], (layer, me * rows, 0), (1, rows, weights[k].shape[2]))[0].astype(F32)
                nw, nm, nv = adamw(mine, m[k][layer], v[k][layer], grads[k][layer].astype(F32) * factor)
                made.append((nm, nv))
                from_left, from_right = lax.ppermute(nw, "dp", to_right), lax.ppermute(nw, "dp", to_left)
                direct[k, layer] = (from_left, from_right)
                blocks += [nw, from_left, from_right]
                where += [(k, layer, 0, 0), (k, layer, n - 1, 0), (k, layer, 1, 0)]
            new_m.append(jnp.stack([nm for nm, _ in made]))
            new_v.append(jnp.stack([nv for _, nv in made]))
        shapes = [w.shape for w in weights]
        whole = place(blocks, where, shapes, (), "place")
        blocks, where = [], []
        for (k, layer), (from_left, from_right) in direct.items():
            half = from_left.shape[0] // 2
            blocks += [lax.ppermute(from_left[:half], "dp", to_right), lax.ppermute(from_right[half:], "dp", to_left)]
            where += [(k, layer, 2, 0), (k, layer, 2, half)]
        whole = place(blocks, where, shapes, whole, "place_far")
        return (*whole, *new_m, *new_v)

    whole, rows = P(None, None, None), P(None, "dp", None)
    return jax.shard_map(
        body,
        mesh=mesh,
        in_specs=(P(("rep", "dp")),) * 2 + (whole,) * 3 + (rows,) * 6,
        out_specs=(P("rep"),) * 3 + (P("rep", "dp"),) * 6,
        check_vma=False,
    )
```

```python
import functools

import jax
import jax.numpy as jnp
from jax import lax
from jax.experimental import pallas as pl
from jax.experimental.pallas import tpu as pltpu
from jax.sharding import PartitionSpec as P

F32, BF16 = jnp.float32, jnp.bfloat16
VMEM_BYTES = 66_000_000
NN = (((1,), (0,)), ((), ()))
NT = (((1,), (1,)), ((), ()))
TN = (((0,), (0,)), ((), ()))


def dot(a, b, dims=NN):
    return lax.dot_general(a, b, dims, preferred_element_type=F32)


def params(**more):
    return pltpu.CompilerParams(vmem_limit_bytes=VMEM_BYTES, **more)


def cost(flops, nbytes):
    return pl.CostEstimate(flops=flops, bytes_accessed=nbytes, transcendentals=0)


def tokens_spec(tile, width):
    return pl.BlockSpec((tile, width), lambda i: (i, 0))


def weight_spec(w, layer):
    return pl.BlockSpec((None, *w.shape[1:]), lambda i: (layer, 0, 0), pipeline_mode=pl.Buffered(1))


def scale_of(wide):
    return lax.rsqrt(jnp.mean(wide * wide, -1, keepdims=True) + 1e-6)


def gated(gate, up):
    sig = 0.5 * jnp.tanh(0.5 * gate) + 0.5
    act = gate * sig
    return act, up * (sig + act * (1.0 - sig)), (act * up).astype(BF16)


def first_kernel(chunk, x_ref, wg, wu, wd, act_ref, slope_ref, hid_ref, h1_ref, a_ref):
    wide = x_ref[...].astype(F32)
    a = (wide * scale_of(wide)).astype(BF16)
    a_ref[...] = a
    for c in range(0, wg.shape[1], chunk):
        at = pl.ds(c, chunk)
        act, slope, hid = gated(dot(a, wg[:, at]), dot(a, wu[:, at]))
        act_ref[:, at] = act
        slope_ref[:, at] = slope
        hid_ref[:, at] = hid
    y = dot(hid_ref[...], wd[...]).astype(BF16)
    h1_ref[...] = (wide + y.astype(F32)).astype(BF16)


def first(x, wg, wu, wd, tile=512, chunk=512):
    t, d = x.shape
    f = wg.shape[2]
    return pl.pallas_call(
        functools.partial(first_kernel, chunk),
        grid=(t // tile,),
        in_specs=[tokens_spec(tile, d), weight_spec(wg, 0), weight_spec(wu, 0), weight_spec(wd, 0)],
        out_specs=[tokens_spec(tile, f)] * 3 + [tokens_spec(tile, d)] * 2,
        out_shape=[
            jax.ShapeDtypeStruct((t, f), F32),
            jax.ShapeDtypeStruct((t, f), F32),
            jax.ShapeDtypeStruct((t, f), BF16),
            jax.ShapeDtypeStruct((t, d), BF16),
            jax.ShapeDtypeStruct((t, d), BF16),
        ],
        compiler_params=params(),
        cost_estimate=cost(6 * t * d * f, 10 * t * f),
        name="first",
    )(x, wg, wu, wd)


def second_kernel(chunk, h_ref, dy_ref, wg, wu, wd, hid_ref, dgate_ref, dup_ref, a_ref):
    wide = h_ref[...].astype(F32)
    a = (wide * scale_of(wide)).astype(BF16)
    a_ref[...] = a
    dy = dy_ref[...]
    for c in range(0, wg.shape[1], chunk):
        at = pl.ds(c, chunk)
        act, slope, hid = gated(dot(a, wg[:, at]), dot(a, wu[:, at]))
        hid_ref[:, at] = hid
        dhid = dot(dy, wd[at, :], NT).astype(BF16).astype(F32)
        dgate_ref[:, at] = (dhid * slope).astype(BF16)
        dup_ref[:, at] = (dhid * act).astype(BF16)


def second(h, dy, wg, wu, wd, tile=512, chunk=512):
    t, d = h.shape
    f = wg.shape[2]
    return pl.pallas_call(
        functools.partial(second_kernel, chunk),
        grid=(t // tile,),
        in_specs=[tokens_spec(tile, d)] * 2 + [weight_spec(wg, 1), weight_spec(wu, 1), weight_spec(wd, 1)],
        out_specs=[tokens_spec(tile, f)] * 3 + [tokens_spec(tile, d)],
        out_shape=[jax.ShapeDtypeStruct((t, f), BF16)] * 3 + [jax.ShapeDtypeStruct((t, d), BF16)],
        compiler_params=params(),
        cost_estimate=cost(6 * t * d * f, 6 * t * f),
        name="second",
    )(h, dy, wg, wu, wd)


N = 4


def back_kernel(axis, tile, rows_tile, *refs):
    (dy, a1, hid1, dgate1, dup1, h1, act0, slope0, hid0, a0, wg, wu, wd), refs = refs[:13], refs[13:]
    (gd0, gd1, ggu0, ggu1, total_ref, dgate0, dup0), refs = refs[:7], refs[7:]
    a_buf, b_buf, wg_buf, wu_buf, wd_buf, dgate_buf, dup_buf, act_buf, slope_buf, h_buf, dgate_out, dup_out = refs[:12]
    term, in1_l, in1_r, in2_l, in2_r, norms = refs[12:18]
    a_sem, b_sem, w_sem, tile_sem, out_sem, ready, norm_sem, send_sem, recv_sem = refs[18:]
    steps = hid1.shape[1] // tile
    part = tile // N
    me = lax.axis_index(axis)
    right, left, across = ((me + k) % N for k in (1, 3, 2))
    mesh_id = pl.DeviceIdType.MESH
    full = [term[kind].shape[1] // N for kind in range(2)]
    half = [f // 2 for f in full]

    def load_a(source, which, sem):
        return pltpu.make_async_copy(source, a_buf.at[which], a_sem.at[sem])

    def load_b(source, j, slot, flip):
        stride, first = (source.shape[1] // N, j * part) if flip else (part, j * tile)
        return [
            pltpu.make_async_copy(
                source.at[:, pl.ds(pl.multiple_of(first + q * stride, part), part)],
                b_buf.at[slot, :, pl.ds(q * part, part)],
                b_sem.at[slot, q],
            )
            for q in range(N)
        ]

    def start(copies):
        for one in copies:
            one.start()

    def rows(kind, device, start, size):
        return pl.ds(pl.multiple_of(device * full[kind] + start, 16), size)

    def sends(kind, at, wanted):
        f, h = full[kind], half[kind]
        low, high = pl.ds(0, h), pl.ds(h, f - h)
        plan = (
            (across, 0, in1_l, pl.ds(0, h), right),
            (across, h, in1_r, pl.ds(0, h), left),
            (right, h, in2_l, high, right),
            (left, 0, in2_r, low, left),
            (right, 0, in2_l, low, right),
            (left, h, in2_r, high, left),
        )
        s = at if kind else steps + at
        made = []
        for which in wanted:
            of, first, into, to, peer = plan[which]
            made.append(
                pltpu.make_async_remote_copy(
                    src_ref=term[kind].at[at, rows(kind, of, first, h)],
                    dst_ref=into[kind].at[at, to],
                    send_sem=send_sem.at[which, s],
                    recv_sem=recv_sem.at[which, s],
                    device_id={axis: peer},
                    device_id_type=mesh_id,
                )
            )
        return made

    def pass_on(kind, at):
        arrived = sends(kind, at, (0, 1))
        onward = sends(kind, at, (4, 5))
        for one, then, of, first, got in ((arrived[0], onward[0], right, 0, in1_l), (arrived[1], onward[1], left, half[kind], in1_r)):
            one.wait_recv()
            here = rows(kind, of, first, half[kind])
            term[kind][at, here, :] = (term[kind][at, here, :].astype(F32) + got[kind][at].astype(F32)).astype(BF16)
            then.start()

    def finish(kind, at, gd, ggu):
        for one in sends(kind, at, (2, 3, 4, 5)):
            one.wait_recv()
        f = full[kind]
        g = term[kind][at, rows(kind, me, 0, f), :].astype(F32) + in2_l[kind][at].astype(F32) + in2_r[kind][at].astype(F32)
        g = g.astype(BF16)
        if kind:
            gd[pl.ds(pl.multiple_of(at * f, f), f), :] = g
        else:
            ggu[at // steps, :, pl.ds(pl.multiple_of(at % steps * tile, tile), tile)] = g
        square = g.astype(F32) * g.astype(F32)
        square = jnp.sum(square.reshape(-1, 8, square.shape[1]), 0)
        total_ref[...] += sum(square[:, c : c + 128] for c in range(0, square.shape[1], 128))

    def drain(kind, count):
        def one_step(at, _):
            for one in sends(kind, at, range(6)):
                one.wait_send()
            return 0

        lax.fori_loop(0, count, one_step, 0)

    def gradients(hid, dgate, dup, next_hid, before_first, gd, ggu):
        def down(j, _):
            slot = j % 2
            for one in load_b(hid, j, slot, True):
                one.wait()

            @pl.when(j < steps - 1)
            def _():
                start(load_b(hid, j + 1, 1 - slot, True))

            @pl.when(j == steps - 1)
            def _():
                start(load_b(dgate, 0, 1 - slot, False))

            term[1][j] = dot(a_buf[0], b_buf[slot], TN).T.astype(BF16)

            @pl.when(j == 0)
            def _():
                before_first()

            start(sends(1, j, range(4)))
            return 0

        lax.fori_loop(0, steps, down, 0)
        load_a(a1, 1, 1).wait()

        def gate_up(i, _):
            slot = i % 2
            for one in load_b(dgate, i % steps, slot, False):
                one.wait()

            @pl.when(i < steps - 1)
            def _():
                start(load_b(dgate, i + 1, 1 - slot, False))

            @pl.when((i >= steps - 1) & (i < 2 * steps - 1))
            def _():
                start(load_b(dup, i + 1 - steps, 1 - slot, False))

            if next_hid is not None:

                @pl.when(i == 2 * steps - 1)
                def _():
                    start(load_b(next_hid, 0, 1 - slot, True))

            term[0][i] = dot(a_buf[1], b_buf[slot], TN).astype(BF16)
            start(sends(0, i, range(4)))

            @pl.when(i < steps)
            def _():
                pass_on(1, i)

            @pl.when(i >= steps)
            def _():
                pass_on(0, i - steps)
                finish(1, i - steps, gd, ggu)

            return 0

        lax.fori_loop(0, 2 * steps, gate_up, 0)

    load_a(dy, 0, 0).start()
    start(load_b(hid1, 0, 0, True))
    load_a(a1, 1, 1).start()
    barrier = pltpu.get_barrier_semaphore()
    for peer in (right, left, across):
        pl.semaphore_signal(barrier, inc=1, device_id={axis: peer}, device_id_type=mesh_id)
    total_ref[...] = jnp.zeros_like(total_ref)
    weights = [
        pltpu.make_async_copy(wg.at[1], wg_buf, w_sem.at[0]),
        pltpu.make_async_copy(wu.at[1], wu_buf, w_sem.at[1]),
        pltpu.make_async_copy(wd.at[0], wd_buf, w_sem.at[2]),
    ]

    def tile_loads(i, slot):
        at = pl.ds(pl.multiple_of(i * rows_tile, rows_tile), rows_tile)
        pairs = ((dgate1, dgate_buf), (dup1, dup_buf), (act0, act_buf), (slope0, slope_buf), (h1, h_buf))
        return [pltpu.make_async_copy(a.at[at], b.at[slot], tile_sem.at[slot, k]) for k, (a, b) in enumerate(pairs)]

    def tile_stores(i, slot):
        at = pl.ds(pl.multiple_of(i * rows_tile, rows_tile), rows_tile)
        pairs = ((dgate_out, dgate0), (dup_out, dup0))
        return [pltpu.make_async_copy(a.at[slot], b.at[at], out_sem.at[slot, k]) for k, (a, b) in enumerate(pairs)]

    load_a(dy, 0, 0).wait()
    start(weights)
    start(tile_loads(0, 0))
    gradients(hid1, dgate1, dup1, hid0, lambda: pl.semaphore_wait(barrier, 3), gd1, ggu1)

    load_a(a0, 1, 1).start()
    for one in weights:
        one.wait()
    tiles = a_buf.shape[1] // rows_tile
    chunk = tile

    def tile_back(i, _):
        slot = i % 2
        at = pl.ds(pl.multiple_of(i * rows_tile, rows_tile), rows_tile)
        for one in tile_loads(i, slot):
            one.wait()

        @pl.when(i < tiles - 1)
        def _():
            start(tile_loads(i + 1, 1 - slot))

        @pl.when(i >= 2)
        def _():
            for one in tile_stores(i - 2, slot):
                one.wait()

        da = dot(dgate_buf[slot], wg_buf[...], NT).astype(BF16) + dot(dup_buf[slot], wu_buf[...], NT).astype(BF16)
        da = da.astype(F32)
        wide = h_buf[slot].astype(F32)
        scale = scale_of(wide)
        along = jnp.mean(da * wide, -1, keepdims=True)
        dn = da * scale - wide * (scale * scale * scale * along)
        dh = (a_buf[0, at, :].astype(F32) + dn.astype(BF16).astype(F32)).astype(BF16)
        a_buf[0, at, :] = dh
        for c in range(0, wd_buf.shape[0], chunk):
            to = pl.ds(c, chunk)
            dhid = dot(dh, wd_buf[to, :], NT).astype(BF16).astype(F32)
            dgate_out[slot, :, to] = (dhid * slope_buf[slot, :, to]).astype(BF16)
            dup_out[slot, :, to] = (dhid * act_buf[slot, :, to]).astype(BF16)
        start(tile_stores(i, slot))

        @pl.when(i < steps)
        def _():
            pass_on(0, steps + i)

        @pl.when(i < 2 * steps)
        def _():
            finish(0, i, gd1, ggu1)

        @pl.when(i == 2 * steps)
        def _():
            for peer in (right, left):
                pl.semaphore_signal(ready, inc=1, device_id={axis: peer}, device_id_type=mesh_id)

        return 0

    lax.fori_loop(0, tiles, tile_back, 0)
    for i in (tiles - 2, tiles - 1):
        for one in tile_stores(i, i % 2):
            one.wait()
    drain(1, steps)
    drain(0, 2 * steps)

    gradients(hid0, dgate0, dup0, None, lambda: pl.semaphore_wait(ready, 2), gd0, ggu0)

    def rest(i, _):
        pass_on(0, steps + i)
        finish(0, i, gd0, ggu0)
        return 0

    def final(i, _):
        finish(0, steps + i, gd0, ggu0)
        return 0

    lax.fori_loop(0, steps, rest, 0)
    lax.fori_loop(0, steps, final, 0)

    norms[3] = total_ref[...]
    copies = [
        pltpu.make_async_remote_copy(
            src_ref=norms.at[3],
            dst_ref=norms.at[to],
            send_sem=norm_sem.at[0, to],
            recv_sem=norm_sem.at[1, to],
            device_id={axis: peer},
            device_id_type=mesh_id,
        )
        for to, peer in enumerate((right, left, across))
    ]
    start(copies)
    drain(1, steps)
    drain(0, 2 * steps)
    for one in copies:
        one.wait()
    total_ref[...] = (norms[0] + norms[1]) + (norms[2] + norms[3])


def back(dy, a1, hid1, dgate1, dup1, h1, act0, slope0, hid0, a0, wg, wu, wd, tile=512, rows_tile=256):
    t, d = dy.shape
    f = hid1.shape[1]
    steps = f // tile
    shapes, counts = ((d, tile), (tile, d)), (2 * steps, steps)

    def each(share, dtype=BF16):
        return [pltpu.VMEM((counts[k], shapes[k][0] // share, shapes[k][1]), dtype) for k in range(2)]

    any_spec, vmem_spec = pl.BlockSpec(memory_space=pl.ANY), pl.BlockSpec(memory_space=pltpu.VMEM)
    down, gate_up = jax.ShapeDtypeStruct((f // N, d), BF16), jax.ShapeDtypeStruct((2, d // N, f), BF16)
    return pl.pallas_call(
        functools.partial(back_kernel, "dp", tile, rows_tile),
        in_specs=[any_spec] * 13,
        out_specs=[vmem_spec] * 5 + [any_spec] * 2,
        out_shape=[down, down, gate_up, gate_up, jax.ShapeDtypeStruct((8, 128), F32)] + [jax.ShapeDtypeStruct((t, f), BF16)] * 2,
        scratch_shapes=[
            pltpu.VMEM((2, t, d), BF16),
            pltpu.VMEM((2, t, tile), BF16),
            pltpu.VMEM((d, f), BF16),
            pltpu.VMEM((d, f), BF16),
            pltpu.VMEM((f, d), BF16),
            pltpu.VMEM((2, rows_tile, f), BF16),
            pltpu.VMEM((2, rows_tile, f), BF16),
            pltpu.VMEM((2, rows_tile, f), F32),
            pltpu.VMEM((2, rows_tile, f), F32),
            pltpu.VMEM((2, rows_tile, d), BF16),
            pltpu.VMEM((2, rows_tile, f), BF16),
            pltpu.VMEM((2, rows_tile, f), BF16),
            each(1),
            each(2 * N),
            each(2 * N),
            each(N),
            each(N),
            pltpu.VMEM((4, 8, 128), F32),
            pltpu.SemaphoreType.DMA((2,)),
            pltpu.SemaphoreType.DMA((2, N)),
            pltpu.SemaphoreType.DMA((3,)),
            pltpu.SemaphoreType.DMA((2, 5)),
            pltpu.SemaphoreType.DMA((2, 2)),
            pltpu.SemaphoreType.REGULAR,
            pltpu.SemaphoreType.DMA((2, 3)),
            pltpu.SemaphoreType.DMA((6, 3 * steps)),
            pltpu.SemaphoreType.DMA((6, 3 * steps)),
        ],
        compiler_params=pltpu.CompilerParams(vmem_limit_bytes=67_000_000, collective_id=1, has_side_effects=True),
        cost_estimate=cost(18 * t * d * f, 40 * t * f),
        name="back",
    )(dy, a1, hid1, dgate1, dup1, h1, act0, slope0, hid0, a0, wg, wu, wd)[:5]


def adamw(w, m, v, g):
    m = 0.9 * m + 0.1 * g
    v = 0.95 * v + 0.05 * g * g
    step = m * lax.rsqrt(v + 1e-8) + 0.1 * w
    return (w - 0.02 * step).astype(BF16), m, v


def place_kernel(axis, where, *refs):
    blocks, refs = refs[: len(where)], refs[len(where) :]
    outs, sems = refs[-4:-1], refs[-1]
    me = lax.axis_index(axis)
    copies = []
    for k, (matrix, layer, shift, start) in enumerate(where):
        rows = outs[matrix].shape[1] // 4
        at = ((me + shift) % 4) * rows + start
        size = blocks[k].shape[0]
        copies.append(pltpu.make_async_copy(blocks[k], outs[matrix].at[layer, pl.ds(pl.multiple_of(at, 16), size), :], sems.at[k]))
    for one in copies:
        one.start()
    for one in copies:
        one.wait()


def place(blocks, where, shapes, into, name):
    any_spec, vmem_spec = pl.BlockSpec(memory_space=pl.ANY), pl.BlockSpec(memory_space=pltpu.VMEM)
    into = list(into)
    return pl.pallas_call(
        functools.partial(place_kernel, "dp", where),
        in_specs=[vmem_spec] * len(blocks) + [any_spec] * len(into),
        out_specs=[any_spec] * 3,
        out_shape=[jax.ShapeDtypeStruct(s, BF16) for s in shapes],
        scratch_shapes=[pltpu.SemaphoreType.DMA((len(blocks),))],
        input_output_aliases={len(blocks) + k: k for k in range(len(into))},
        compiler_params=params(),
        cost_estimate=cost(1000, sum(b.size for b in blocks) * 4),
        name=name,
    )(*blocks, *into)


def solution(mesh):
    n = mesh.shape["dp"]
    to_right = [(i, (i + 1) % n) for i in range(n)]
    to_left = [(i, (i - 1) % n) for i in range(n)]

    def body(x, dy, wg, wu, wd, *moments):
        m, v = moments[:3], moments[3:]
        x, dy = x[0], dy[0]
        act0, slope0, hid0, h1, a0 = first(x, wg, wu, wd)
        hid1, dgate1, dup1, a1 = second(h1, dy, wg, wu, wd)
        gd0, gd1, ggu0, ggu1, total = back(dy, a1, hid1, dgate1, dup1, h1, act0, slope0, hid0, a0, wg, wu, wd)
        count = sum(w.size for w in (wg, wu, wd))
        factor = jnp.minimum(1.0, 0.5 * lax.rsqrt(jnp.sum(total) / count + 1e-30))
        me = lax.axis_index("dp")
        grads = ((ggu0[0], ggu1[0]), (ggu0[1], ggu1[1]), (gd0, gd1))
        weights = (wg, wu, wd)
        new_m, new_v, blocks, where = [], [], [], []
        direct = {}
        for k in (0, 1, 2):
            rows = m[k].shape[1]
            made = []
            for layer in range(2):
                mine = lax.dynamic_slice(weights[k], (layer, me * rows, 0), (1, rows, weights[k].shape[2]))[0].astype(F32)
                nw, nm, nv = adamw(mine, m[k][layer], v[k][layer], grads[k][layer].astype(F32) * factor)
                made.append((nm, nv))
                from_left, from_right = lax.ppermute(nw, "dp", to_right), lax.ppermute(nw, "dp", to_left)
                direct[k, layer] = (from_left, from_right)
                blocks += [nw, from_left, from_right]
                where += [(k, layer, 0, 0), (k, layer, n - 1, 0), (k, layer, 1, 0)]
            new_m.append(jnp.stack([nm for nm, _ in made]))
            new_v.append(jnp.stack([nv for _, nv in made]))
        shapes = [w.shape for w in weights]
        whole = place(blocks, where, shapes, (), "place")
        blocks, where = [], []
        for (k, layer), (from_left, from_right) in direct.items():
            half = from_left.shape[0] // 2
            blocks += [lax.ppermute(from_left[:half], "dp", to_right), lax.ppermute(from_right[half:], "dp", to_left)]
            where += [(k, layer, 2, 0), (k, layer, 2, half)]
        whole = place(blocks, where, shapes, whole, "place_far")
        return (*whole, *new_m, *new_v)

    whole, rows = P(None, None, None), P(None, "dp", None)
    return jax.shard_map(
        body,
        mesh=mesh,
        in_specs=(P(("rep", "dp")),) * 2 + (whole,) * 3 + (rows,) * 6,
        out_specs=(P("rep"),) * 3 + (P("rep", "dp"),) * 6,
        check_vma=False,
    )
```

```python
import functools

import jax
import jax.numpy as jnp
from jax import lax
from jax.experimental import pallas as pl
from jax.experimental.pallas import tpu as pltpu
from jax.sharding import PartitionSpec as P


F32, BF16 = jnp.float32, jnp.bfloat16
VMEM_BYTES = 66_000_000
NN = (((1,), (0,)), ((), ()))
NT = (((1,), (1,)), ((), ()))


def dot(a, b, dims=NN):
    return lax.dot_general(a, b, dims, preferred_element_type=F32)


def params(**more):
    return pltpu.CompilerParams(vmem_limit_bytes=VMEM_BYTES, **more)


def cost(flops, nbytes):
    return pl.CostEstimate(flops=flops, bytes_accessed=nbytes, transcendentals=0)


def tokens_spec(tile, width):
    return pl.BlockSpec((tile, width), lambda i: (i, 0))


BLOCK = 512


def blocks_spec(tile, width):
    return pl.BlockSpec((width // BLOCK, tile, BLOCK), lambda i: (0, i, 0))


def blocks_shape(tokens, width):
    return jax.ShapeDtypeStruct((width // BLOCK, tokens, BLOCK), BF16)


def spread(hid_ref, which, hid):
    parts = hid_ref.shape[0]
    size = BLOCK // parts
    for j in range(parts):
        hid_ref[j, :, which * size : (which + 1) * size] = hid[:, j * size : (j + 1) * size]


def across_spec(tile, width):
    return pl.BlockSpec((width, tile), lambda i: (0, i))


def weight_spec(w, layer):
    return pl.BlockSpec((None, *w.shape[1:]), lambda i: (layer, 0, 0), pipeline_mode=pl.Buffered(1))


def scale_of(wide):
    return lax.rsqrt(jnp.mean(wide * wide, -1, keepdims=True) + 1e-6)


def gated(gate, up):
    sig = 0.5 * jnp.tanh(0.5 * gate) + 0.5
    act = gate * sig
    return act, up * (sig + act * (1.0 - sig)), (act * up).astype(BF16)


def front_kernel(x_ref, dy_ref, wg0, wu0, wd0, wg1, wu1, wd1, act_ref, slope_ref, hid0_ref, h1_ref, a0_ref, hid1_ref, dgate_ref, dup_ref, a1_ref, dy_out, whole_ref):
    wide = x_ref[...].astype(F32)
    a = (wide * scale_of(wide)).astype(BF16)
    a0_ref[...] = a.T
    for c in range(wg0.shape[1] // BLOCK):
        at = pl.ds(c * BLOCK, BLOCK)
        act, slope, hid = gated(dot(a, wg0[:, at]), dot(a, wu0[:, at]))
        act_ref[:, at] = act
        slope_ref[:, at] = slope
        whole_ref[:, at] = hid
        spread(hid0_ref, c, hid)
    y = dot(whole_ref[...], wd0[...]).astype(BF16)
    h = (wide + y.astype(F32)).astype(BF16)
    h1_ref[...] = h
    wide = h.astype(F32)
    a = (wide * scale_of(wide)).astype(BF16)
    a1_ref[...] = a.T
    dy = dy_ref[...]
    dy_out[...] = dy.T
    for c in range(wg1.shape[1] // BLOCK):
        at = pl.ds(c * BLOCK, BLOCK)
        act, slope, hid = gated(dot(a, wg1[:, at]), dot(a, wu1[:, at]))
        spread(hid1_ref, c, hid)
        dhid = dot(dy, wd1[at, :], NT).astype(BF16).astype(F32)
        dgate_ref[c] = (dhid * slope).astype(BF16)
        dup_ref[c] = (dhid * act).astype(BF16)


def front(x, dy, wg, wu, wd, tile=256):
    t, d = x.shape
    f = wg.shape[2]
    tokens, turned, wide = tokens_spec(tile, d), across_spec(tile, d), tokens_spec(tile, f)
    blocks = blocks_spec(tile, f)
    token_shape, turned_shape = jax.ShapeDtypeStruct((t, d), BF16), jax.ShapeDtypeStruct((d, t), BF16)
    wide_shape, block_shape = jax.ShapeDtypeStruct((t, f), F32), blocks_shape(t, f)
    return pl.pallas_call(
        front_kernel,
        grid=(t // tile,),
        in_specs=[tokens] * 2 + [weight_spec(w, layer) for layer in range(2) for w in (wg, wu, wd)],
        out_specs=[wide, wide, blocks, tokens, turned, blocks, blocks, blocks, turned, turned],
        out_shape=[wide_shape] * 2 + [block_shape, token_shape, turned_shape] + [block_shape] * 3 + [turned_shape] * 2,
        scratch_shapes=[pltpu.VMEM((tile, f), BF16)],
        compiler_params=pltpu.CompilerParams(vmem_limit_bytes=67_000_000),
        cost_estimate=cost(12 * t * d * f, 16 * t * f),
        name="front",
    )(x, dy, wg, wu, wd, wg, wu, wd)


N = 4


def back_kernel(axis, tile, rows_tile, *refs):
    (dy, dy_t, a1, hid1, dgate1, dup1, h1, act0, slope0, hid0, a0, wg, wu, wd), refs = refs[:14], refs[14:]
    (gd0, gd1, ggu0, ggu1, total_ref, dgate0, dup0), refs = refs[:7], refs[7:]
    a_buf, b_buf, wg_buf, wu_buf, wd_buf, dgate_buf, dup_buf, act_buf, slope_buf, h_buf, dy_buf, dgate_out, dup_out = refs[:13]
    term, got_l, got_r, sum_l, sum_r, stage, norms = refs[13:20]
    a_sem, b_sem, w_sem, tile_sem, out_sem, ready, norm_sem, send_sem, recv_sem = refs[20:]
    steps = hid1.shape[0]
    me = lax.axis_index(axis)
    right, left, across = ((me + k) % N for k in (1, 3, 2))
    mesh_id = pl.DeviceIdType.MESH

    def load_a(source, which, sem):
        return pltpu.make_async_copy(source, a_buf.at[which], a_sem.at[sem])

    def load_b(source, j, slot):
        return pltpu.make_async_copy(source.at[j], b_buf.at[slot], b_sem.at[slot])

    def start(copies):
        for one in copies:
            one.start()

    halves = ((across, 0), (right, 1), (across, 1), (left, 0), (right, 0), (left, 1), (me, 0), (me, 1))

    def put(kind, step, out):
        stage[kind][...] = (out.T if kind else out).astype(BF16)
        size = term[kind].shape[2]
        for place, (device, which) in enumerate(halves):
            rows = pl.ds(pl.multiple_of(device * 2 * size + which * size, 16), size)
            term[kind][step, place] = stage[kind][rows, :]

    def sends(kind, at, wanted):
        plan = (
            (pl.ds(0, 2), got_l, right),
            (pl.ds(2, 2), got_r, left),
            (4, sum_l, right),
            (5, sum_r, left),
        )
        s = at if kind else steps + at
        made = []
        for which in wanted:
            of, into, peer = plan[which]
            made.append(
                pltpu.make_async_remote_copy(
                    src_ref=term[kind].at[at, of],
                    dst_ref=into[kind].at[at],
                    send_sem=send_sem.at[which, s],
                    recv_sem=recv_sem.at[which, s],
                    device_id={axis: peer},
                    device_id_type=mesh_id,
                )
            )
        return made

    def pass_on(kind, at):
        arrived = sends(kind, at, (0, 1))
        onward = sends(kind, at, (2, 3))
        for one, then, place, got in ((arrived[0], onward[0], 4, got_l), (arrived[1], onward[1], 5, got_r)):
            one.wait_recv()
            term[kind][at, place] = (term[kind][at, place].astype(F32) + got[kind][at, 0].astype(F32)).astype(BF16)
            then.start()

    def finish(kind, at, gd, ggu):
        for one in sends(kind, at, (2, 3)):
            one.wait_recv()
        low = term[kind][at, 6].astype(F32) + sum_l[kind][at].astype(F32) + got_r[kind][at, 1].astype(F32)
        high = term[kind][at, 7].astype(F32) + got_l[kind][at, 1].astype(F32) + sum_r[kind][at].astype(F32)
        for which, g in enumerate((low, high)):
            g = g.astype(BF16)
            size = g.shape[0]
            if kind:
                gd[pl.ds(pl.multiple_of(at * 2 * size + which * size, size), size), :] = g
            else:
                columns = pl.ds(pl.multiple_of(at % steps * tile, tile), tile)
                ggu[at // steps, pl.ds(which * size, size), columns] = g
            square = g.astype(F32) * g.astype(F32)
            square = jnp.sum(square.reshape(-1, 8, square.shape[1]), 0)
            total_ref[...] += sum(square[:, c : c + 128] for c in range(0, square.shape[1], 128))

    def drain(kind, count):
        def one_step(at, _):
            for one in sends(kind, at, range(4)):
                one.wait_send()
            return 0

        lax.fori_loop(0, count, one_step, 0)

    def gradients(hid, dgate, dup, next_hid, before_first, gd, ggu):
        def down(j, _):
            slot = j % 2
            load_b(hid, j, slot).wait()
            put(1, j, dot(a_buf[0], b_buf[slot]))

            @pl.when(j < steps - 2)
            def _():
                load_b(hid, j + 2, slot).start()

            @pl.when(j >= steps - 2)
            def _():
                load_b(dgate, j + 2 - steps, slot).start()

            @pl.when(j == 0)
            def _():
                before_first()

            start(sends(1, j, (0, 1)))
            return 0

        lax.fori_loop(0, steps, down, 0)
        load_a(a1, 1, 1).wait()

        def gate_up(i, _):
            slot = i % 2
            load_b(dgate, i % steps, slot).wait()
            put(0, i, dot(a_buf[1], b_buf[slot]))

            @pl.when(i < steps - 2)
            def _():
                load_b(dgate, i + 2, slot).start()

            @pl.when((i >= steps - 2) & (i < 2 * steps - 2))
            def _():
                load_b(dup, i + 2 - steps, slot).start()

            if next_hid is not None:

                @pl.when(i >= 2 * steps - 2)
                def _():
                    load_b(next_hid, i + 2 - 2 * steps, slot).start()

            start(sends(0, i, (0, 1)))

            @pl.when(i < steps)
            def _():
                pass_on(1, i)

            @pl.when(i >= steps)
            def _():
                pass_on(0, i - steps)
                finish(1, i - steps, gd, ggu)

            return 0

        lax.fori_loop(0, 2 * steps, gate_up, 0)

    load_a(dy_t, 0, 0).start()
    load_b(hid1, 0, 0).start()
    load_b(hid1, 1, 1).start()
    load_a(a1, 1, 1).start()
    barrier = pltpu.get_barrier_semaphore()
    for peer in (right, left, across):
        pl.semaphore_signal(barrier, inc=1, device_id={axis: peer}, device_id_type=mesh_id)
    total_ref[...] = jnp.zeros_like(total_ref)
    weights = [
        pltpu.make_async_copy(wg.at[1], wg_buf, w_sem.at[0]),
        pltpu.make_async_copy(wu.at[1], wu_buf, w_sem.at[1]),
        pltpu.make_async_copy(wd.at[0], wd_buf, w_sem.at[2]),
    ]

    def tile_loads(i, slot):
        at = pl.ds(pl.multiple_of(i * rows_tile, rows_tile), rows_tile)
        blocks = [(one.at[:, at], buf) for one, buf in ((dgate1, dgate_buf), (dup1, dup_buf))]
        pairs = ((act0, act_buf), (slope0, slope_buf), (h1, h_buf), (dy, dy_buf))
        blocks += [(one.at[at], buf) for one, buf in pairs]
        return [pltpu.make_async_copy(a, b.at[slot], tile_sem.at[slot, k]) for k, (a, b) in enumerate(blocks)]

    def tile_stores(i, slot):
        at = pl.ds(pl.multiple_of(i * rows_tile, rows_tile), rows_tile)
        pairs = ((dgate_out, dgate0), (dup_out, dup0))
        return [pltpu.make_async_copy(a.at[slot], b.at[:, at], out_sem.at[slot, k]) for k, (a, b) in enumerate(pairs)]

    load_a(dy_t, 0, 0).wait()
    start(weights)
    start(tile_loads(0, 0))
    gradients(hid1, dgate1, dup1, hid0, lambda: pl.semaphore_wait(barrier, 3), gd1, ggu1)

    load_a(a0, 1, 1).start()
    for one in weights:
        one.wait()
    tiles = a_buf.shape[2] // rows_tile

    def tile_back(i, _):
        slot = i % 2
        at = pl.ds(pl.multiple_of(i * rows_tile, rows_tile), rows_tile)
        for one in tile_loads(i, slot):
            one.wait()

        @pl.when(i < tiles - 1)
        def _():
            start(tile_loads(i + 1, 1 - slot))

        @pl.when(i >= 2)
        def _():
            for one in tile_stores(i - 2, slot):
                one.wait()

        da = [
            sum(dot(w[:, c * tile : (c + 1) * tile], by[slot, c], NT) for c in range(steps)).astype(BF16)
            for w, by in ((wg_buf, dgate_buf), (wu_buf, dup_buf))
        ]
        da = da[0] + da[1]
        da = da.astype(F32).T
        wide = h_buf[slot].astype(F32)
        scale = scale_of(wide)
        along = jnp.mean(da * wide, -1, keepdims=True)
        dn = da * scale - wide * (scale * scale * scale * along)
        dh = (dy_buf[slot].astype(F32) + dn.astype(BF16).astype(F32)).astype(BF16)
        a_buf[0, :, at] = dh.T
        for c in range(steps):
            to = pl.ds(c * tile, tile)
            dhid = dot(dh, wd_buf[to, :], NT).astype(BF16).astype(F32)
            dgate_out[slot, c] = (dhid * slope_buf[slot, :, to]).astype(BF16)
            dup_out[slot, c] = (dhid * act_buf[slot, :, to]).astype(BF16)
        start(tile_stores(i, slot))

        ended = tiles - 2 * steps

        @pl.when((i >= ended - steps) & (i < ended))
        def _():
            pass_on(0, i - ended + 2 * steps)

        @pl.when(i >= ended)
        def _():
            finish(0, i - ended, gd1, ggu1)

        return 0

    lax.fori_loop(0, tiles, tile_back, 0)
    for peer in (right, left):
        pl.semaphore_signal(ready, inc=1, device_id={axis: peer}, device_id_type=mesh_id)
    for i in (tiles - 2, tiles - 1):
        for one in tile_stores(i, i % 2):
            one.wait()
    drain(1, steps)
    drain(0, 2 * steps)

    gradients(hid0, dgate0, dup0, None, lambda: pl.semaphore_wait(ready, 2), gd0, ggu0)

    def rest(i, _):
        pass_on(0, steps + i)
        finish(0, i, gd0, ggu0)
        return 0

    def final(i, _):
        finish(0, steps + i, gd0, ggu0)
        return 0

    lax.fori_loop(0, steps, rest, 0)
    lax.fori_loop(0, steps, final, 0)

    norms[3] = total_ref[...]
    copies = [
        pltpu.make_async_remote_copy(
            src_ref=norms.at[3],
            dst_ref=norms.at[to],
            send_sem=norm_sem.at[0, to],
            recv_sem=norm_sem.at[1, to],
            device_id={axis: peer},
            device_id_type=mesh_id,
        )
        for to, peer in enumerate((right, left, across))
    ]
    start(copies)
    drain(1, steps)
    drain(0, 2 * steps)
    for one in copies:
        one.wait()
    total = jnp.sum((norms[0] + norms[1]) + (norms[2] + norms[3]), keepdims=True)
    factor = jnp.minimum(1.0, 0.5 * lax.rsqrt(total / (3.0 * wg.shape[0] * wg.shape[1] * wg.shape[2]) + 1e-30))
    total_ref[...] = jnp.broadcast_to(factor, total_ref.shape)


def back(dy, dy_t, a1, hid1, dgate1, dup1, h1, act0, slope0, hid0, a0, wg, wu, wd, rows_tile=256):
    t, d = dy.shape
    steps, _, tile = hid1.shape
    f = steps * tile
    shapes, counts = ((d // (2 * N), tile), (tile // (2 * N), d)), (2 * steps, steps)

    def each(*parts):
        return [pltpu.VMEM((counts[k], *parts, *shapes[k]), BF16) for k in range(2)]

    any_spec, vmem_spec = pl.BlockSpec(memory_space=pl.ANY), pl.BlockSpec(memory_space=pltpu.VMEM)
    down, gate_up = jax.ShapeDtypeStruct((f // N, d), BF16), jax.ShapeDtypeStruct((2, d // N, f), BF16)
    return pl.pallas_call(
        functools.partial(back_kernel, "dp", tile, rows_tile),
        in_specs=[any_spec] * 14,
        out_specs=[vmem_spec] * 5 + [any_spec] * 2,
        out_shape=[down, down, gate_up, gate_up, jax.ShapeDtypeStruct((8, 128), F32)] + [blocks_shape(t, f)] * 2,
        scratch_shapes=[
            pltpu.VMEM((2, d, t), BF16),
            pltpu.VMEM((2, t, tile), BF16),
            pltpu.VMEM((d, f), BF16),
            pltpu.VMEM((d, f), BF16),
            pltpu.VMEM((f, d), BF16),
            pltpu.VMEM((2, steps, rows_tile, tile), BF16),
            pltpu.VMEM((2, steps, rows_tile, tile), BF16),
            pltpu.VMEM((2, rows_tile, f), F32),
            pltpu.VMEM((2, rows_tile, f), F32),
            pltpu.VMEM((2, rows_tile, d), BF16),
            pltpu.VMEM((2, rows_tile, d), BF16),
            pltpu.VMEM((2, steps, rows_tile, tile), BF16),
            pltpu.VMEM((2, steps, rows_tile, tile), BF16),
            each(2 * N),
            each(2),
            each(2),
            each(),
            each(),
            [pltpu.VMEM((d, tile), BF16), pltpu.VMEM((tile, d), BF16)],
            pltpu.VMEM((4, 8, 128), F32),
            pltpu.SemaphoreType.DMA((2,)),
            pltpu.SemaphoreType.DMA((2,)),
            pltpu.SemaphoreType.DMA((3,)),
            pltpu.SemaphoreType.DMA((2, 6)),
            pltpu.SemaphoreType.DMA((2, 2)),
            pltpu.SemaphoreType.REGULAR,
            pltpu.SemaphoreType.DMA((2, 3)),
            pltpu.SemaphoreType.DMA((4, 3 * steps)),
            pltpu.SemaphoreType.DMA((4, 3 * steps)),
        ],
        compiler_params=pltpu.CompilerParams(vmem_limit_bytes=67_000_000, collective_id=1, has_side_effects=True),
        cost_estimate=cost(18 * t * d * f, 40 * t * f),
        name="back",
    )(dy, dy_t, a1, hid1, dgate1, dup1, h1, act0, slope0, hid0, a0, wg, wu, wd)[:5]


def adamw(w, m, v, g):
    m = 0.9 * m + 0.1 * g
    v = 0.95 * v + 0.05 * g * g
    step = m * lax.rsqrt(v + 1e-8) + 0.1 * w
    return (w - 0.02 * step).astype(BF16), m, v


def update_kernel(me_ref, factor_ref, g_ref, m_ref, v_ref, w_ref, *refs):
    new_w, new_m, new_v = refs[-3:]
    g = g_ref[...].astype(F32) * factor_ref[0:1, 0:1]
    new_w[...], new_m[...], new_v[...] = adamw(w_ref[...].astype(F32), m_ref[...], v_ref[...], g)


def update(me, factor, g, which, m, v, w, layer, into, blocks=2):
    rows, columns = m.shape[1:]
    size = rows // blocks
    own = pl.BlockSpec((None, size, columns), lambda i, me: (layer, i, 0))
    if g.ndim == 3:
        g_spec = pl.BlockSpec((None, size, columns), lambda i, me: (which, i, 0))
    else:
        g_spec = pl.BlockSpec((size, columns), lambda i, me: (i, 0))
    return pl.pallas_call(
        update_kernel,
        grid_spec=pltpu.PrefetchScalarGridSpec(
            num_scalar_prefetch=1,
            grid=(blocks,),
            in_specs=[
                pl.BlockSpec((8, 128), lambda i, me: (0, 0)),
                g_spec,
                own,
                own,
                pl.BlockSpec((None, size, columns), lambda i, me: (layer, me[0] * blocks + i, 0)),
            ]
            + [pl.BlockSpec(memory_space=pl.ANY)] * len(into),
            out_specs=[pl.BlockSpec((size, columns), lambda i, me: (i, 0)), own, own],
        ),
        out_shape=[jax.ShapeDtypeStruct((rows, columns), BF16)] + [jax.ShapeDtypeStruct(m.shape, F32)] * 2,
        input_output_aliases={6 + k: 1 + k for k in range(len(into))},
        compiler_params=params(),
        cost_estimate=cost(2_000_000_000, 22 * rows * columns),
    )(me, factor, g, m, v, w, *into)


def place_kernel(axis, where, *refs):
    blocks, refs = refs[: len(where)], refs[len(where) :]
    outs, sems = refs[-4:-1], refs[-1]
    me = lax.axis_index(axis)
    copies = []
    for k, (matrix, layer, shift, start) in enumerate(where):
        rows = outs[matrix].shape[1] // 4
        at = ((me + shift) % 4) * rows + start
        size = blocks[k].shape[0]
        copies.append(pltpu.make_async_copy(blocks[k], outs[matrix].at[layer, pl.ds(pl.multiple_of(at, 16), size), :], sems.at[k]))
    for one in copies:
        one.start()
    for one in copies:
        one.wait()


def place(blocks, where, shapes, into):
    any_spec, vmem_spec = pl.BlockSpec(memory_space=pl.ANY), pl.BlockSpec(memory_space=pltpu.VMEM)
    into = list(into)
    return pl.pallas_call(
        functools.partial(place_kernel, "dp", where),
        in_specs=[vmem_spec] * len(blocks) + [any_spec] * len(into),
        out_specs=[any_spec] * 3,
        out_shape=[jax.ShapeDtypeStruct(s, BF16) for s in shapes],
        scratch_shapes=[pltpu.SemaphoreType.DMA((len(blocks),))],
        input_output_aliases={len(blocks) + k: k for k in range(len(into))},
        compiler_params=params(),
        cost_estimate=cost(1000, sum(b.size for b in blocks) * 4),
    )(*blocks, *into)


def solution(mesh):
    n = mesh.shape["dp"]
    to_right = [(i, (i + 1) % n) for i in range(n)]
    to_left = [(i, (i - 1) % n) for i in range(n)]

    def body(x, dy, wg, wu, wd, *moments):
        m, v = moments[:3], moments[3:]
        x, dy = x[0], dy[0]
        act0, slope0, hid0, h1, a0, hid1, dgate1, dup1, a1, dy_t = front(x, dy, wg, wu, wd)
        gd0, gd1, ggu0, ggu1, factor = back(dy, dy_t, a1, hid1, dgate1, dup1, h1, act0, slope0, hid0, a0, wg, wu, wd)
        me = lax.axis_index("dp").astype(jnp.int32).reshape(1)
        weights = (wg, wu, wd)
        new, blocks, where, direct = [(), (), ()], [], [], {}
        for k in range(3):
            for layer, g in enumerate((gd0, gd1) if k == 2 else (ggu0, ggu1)):
                own, *new[k] = update(me, factor, g, k, m[k], v[k], weights[k], layer, new[k])
                from_left = lax.ppermute(own, "dp", to_right)
                from_right = lax.ppermute(own, "dp", to_left)
                direct[k, layer] = (from_left, from_right)
                blocks += [own, from_left, from_right]
                where += [(k, layer, 0, 0), (k, layer, n - 1, 0), (k, layer, 1, 0)]
        shapes = [w.shape for w in weights]
        whole = place(blocks, where, shapes, ())
        far = []
        for (k, layer), (from_left, from_right) in direct.items():
            half = from_left.shape[0] // 2
            far += [
                (lax.ppermute(from_left[:half], "dp", to_right), (k, layer, 2, 0)),
                (lax.ppermute(from_right[half:], "dp", to_left), (k, layer, 2, half)),
            ]
        for part in (far[:8], far[8:]):
            whole = place([one[0] for one in part], [one[1] for one in part], shapes, whole)
        return (*whole, *(one[0] for one in new), *(one[1] for one in new))

    whole, rows = P(None, None, None), P(None, "dp", None)
    return jax.shard_map(
        body,
        mesh=mesh,
        in_specs=(P(("rep", "dp")),) * 2 + (whole,) * 3 + (rows,) * 6,
        out_specs=(P("rep"),) * 3 + (P("rep", "dp"),) * 6,
        check_vma=False,
    )
```

```python
import functools

import jax
import jax.numpy as jnp
from jax import lax
from jax.experimental import pallas as pl
from jax.experimental.pallas import tpu as pltpu
from jax.sharding import PartitionSpec as P


F32, BF16 = jnp.float32, jnp.bfloat16
VMEM_BYTES = 66_000_000
NN = (((1,), (0,)), ((), ()))
NT = (((1,), (1,)), ((), ()))


def dot(a, b, dims=NN):
    return lax.dot_general(a, b, dims, preferred_element_type=F32)


def params(**more):
    return pltpu.CompilerParams(vmem_limit_bytes=VMEM_BYTES, **more)


def cost(flops, nbytes):
    return pl.CostEstimate(flops=flops, bytes_accessed=nbytes, transcendentals=0)


def tokens_spec(tile, width):
    return pl.BlockSpec((tile, width), lambda i: (i, 0))


BLOCK = 512


def blocks_spec(tile, width):
    return pl.BlockSpec((width // BLOCK, tile, BLOCK), lambda i: (0, i, 0))


def blocks_shape(tokens, width):
    return jax.ShapeDtypeStruct((width // BLOCK, tokens, BLOCK), BF16)


def spread(hid_ref, which, hid):
    parts = hid_ref.shape[0]
    size = BLOCK // parts
    for j in range(parts):
        hid_ref[j, :, which * size : (which + 1) * size] = hid[:, j * size : (j + 1) * size]


def across_spec(tile, width):
    return pl.BlockSpec((width, tile), lambda i: (0, i))


def weight_spec(w, layer):
    return pl.BlockSpec((None, *w.shape[1:]), lambda i: (layer, 0, 0), pipeline_mode=pl.Buffered(1))


def scale_of(wide):
    return lax.rsqrt(jnp.mean(wide * wide, -1, keepdims=True) + 1e-6)


def gated(gate, up):
    sig = 0.5 * jnp.tanh(0.5 * gate) + 0.5
    act = gate * sig
    return act, up * (sig + act * (1.0 - sig)), (act * up).astype(BF16)


def front_kernel(x_ref, dy_ref, wg0, wu0, wd0, wg1, wu1, wd1, act_ref, slope_ref, hid0_ref, h1_ref, a0_ref, hid1_ref, dgate_ref, dup_ref, a1_ref, dy_out, whole_ref):
    wide = x_ref[...].astype(F32)
    a = (wide * scale_of(wide)).astype(BF16)
    a0_ref[...] = a.T
    for c in range(wg0.shape[1] // BLOCK):
        at = pl.ds(c * BLOCK, BLOCK)
        act, slope, hid = gated(dot(a, wg0[:, at]), dot(a, wu0[:, at]))
        act_ref[:, at] = act
        slope_ref[:, at] = slope
        whole_ref[:, at] = hid
        spread(hid0_ref, c, hid)
    y = dot(whole_ref[...], wd0[...]).astype(BF16)
    h = (wide + y.astype(F32)).astype(BF16)
    h1_ref[...] = h
    wide = h.astype(F32)
    a = (wide * scale_of(wide)).astype(BF16)
    a1_ref[...] = a.T
    dy = dy_ref[...]
    dy_out[...] = dy.T
    for c in range(wg1.shape[1] // BLOCK):
        at = pl.ds(c * BLOCK, BLOCK)
        act, slope, hid = gated(dot(a, wg1[:, at]), dot(a, wu1[:, at]))
        spread(hid1_ref, c, hid)
        dhid = dot(dy, wd1[at, :], NT).astype(BF16).astype(F32)
        dgate_ref[c] = (dhid * slope).astype(BF16)
        dup_ref[c] = (dhid * act).astype(BF16)


def front(x, dy, wg, wu, wd, tile=256):
    t, d = x.shape
    f = wg.shape[2]
    tokens, turned, wide = tokens_spec(tile, d), across_spec(tile, d), tokens_spec(tile, f)
    blocks = blocks_spec(tile, f)
    token_shape, turned_shape = jax.ShapeDtypeStruct((t, d), BF16), jax.ShapeDtypeStruct((d, t), BF16)
    wide_shape, block_shape = jax.ShapeDtypeStruct((t, f), F32), blocks_shape(t, f)
    return pl.pallas_call(
        front_kernel,
        grid=(t // tile,),
        in_specs=[tokens] * 2 + [weight_spec(w, layer) for layer in range(2) for w in (wg, wu, wd)],
        out_specs=[wide, wide, blocks, tokens, turned, blocks, blocks, blocks, turned, turned],
        out_shape=[wide_shape] * 2 + [block_shape, token_shape, turned_shape] + [block_shape] * 3 + [turned_shape] * 2,
        scratch_shapes=[pltpu.VMEM((tile, f), BF16)],
        compiler_params=pltpu.CompilerParams(vmem_limit_bytes=67_000_000),
        cost_estimate=cost(12 * t * d * f, 16 * t * f),
        name="front",
    )(x, dy, wg, wu, wd, wg, wu, wd)


N = 4


def back_kernel(axis, tile, rows_tile, *refs):
    (dy, dy_t, a1, hid1, dgate1, dup1, h1, act0, slope0, hid0, a0, wg, wu, wd), refs = refs[:14], refs[14:]
    (gd0, gd1, ggu0, ggu1, total_ref, dgate0, dup0), refs = refs[:7], refs[7:]
    a_buf, b_buf, wg_buf, wu_buf, wd_buf, dgate_buf, dup_buf, act_buf, slope_buf, h_buf, dy_buf, dgate_out, dup_out = refs[:13]
    term, got_l, got_r, sum_l, sum_r, stage, norms = refs[13:20]
    a_sem, b_sem, w_sem, tile_sem, out_sem, ready, norm_sem, send_sem, recv_sem = refs[20:]
    steps = hid1.shape[0]
    me = lax.axis_index(axis)
    right, left, across = ((me + k) % N for k in (1, 3, 2))
    mesh_id = pl.DeviceIdType.MESH

    def load_a(source, which, sem):
        return pltpu.make_async_copy(source, a_buf.at[which], a_sem.at[sem])

    def load_b(source, j, slot):
        return pltpu.make_async_copy(source.at[j], b_buf.at[slot], b_sem.at[slot])

    def start(copies):
        for one in copies:
            one.start()

    halves = ((across, 0), (right, 1), (across, 1), (left, 0), (right, 0), (left, 1), (me, 0), (me, 1))

    def put(kind, step, out):
        stage[kind][...] = (out.T if kind else out).astype(BF16)
        size = term[kind].shape[2]
        for place, (device, which) in enumerate(halves):
            rows = pl.ds(pl.multiple_of(device * 2 * size + which * size, 16), size)
            term[kind][step, place] = stage[kind][rows, :]

    def sends(kind, at, wanted):
        plan = (
            (pl.ds(0, 2), got_l, right),
            (pl.ds(2, 2), got_r, left),
            (4, sum_l, right),
            (5, sum_r, left),
        )
        s = at if kind else steps + at
        made = []
        for which in wanted:
            of, into, peer = plan[which]
            made.append(
                pltpu.make_async_remote_copy(
                    src_ref=term[kind].at[at, of],
                    dst_ref=into[kind].at[at],
                    send_sem=send_sem.at[which, s],
                    recv_sem=recv_sem.at[which, s],
                    device_id={axis: peer},
                    device_id_type=mesh_id,
                )
            )
        return made

    def pass_on(kind, at):
        arrived = sends(kind, at, (0, 1))
        onward = sends(kind, at, (2, 3))
        for one, then, place, got in ((arrived[0], onward[0], 4, got_l), (arrived[1], onward[1], 5, got_r)):
            one.wait_recv()
            term[kind][at, place] = (term[kind][at, place].astype(F32) + got[kind][at, 0].astype(F32)).astype(BF16)
            then.start()

    def finish(kind, at, gd, ggu):
        for one in sends(kind, at, (2, 3)):
            one.wait_recv()
        low = term[kind][at, 6].astype(F32) + sum_l[kind][at].astype(F32) + got_r[kind][at, 1].astype(F32)
        high = term[kind][at, 7].astype(F32) + got_l[kind][at, 1].astype(F32) + sum_r[kind][at].astype(F32)
        for which, g in enumerate((low, high)):
            g = g.astype(BF16)
            size = g.shape[0]
            if kind:
                gd[pl.ds(pl.multiple_of(at * 2 * size + which * size, size), size), :] = g
            else:
                columns = pl.ds(pl.multiple_of(at % steps * tile, tile), tile)
                ggu[at // steps, pl.ds(which * size, size), columns] = g
            square = g.astype(F32) * g.astype(F32)
            square = jnp.sum(square.reshape(-1, 8, square.shape[1]), 0)
            total_ref[...] += sum(square[:, c : c + 128] for c in range(0, square.shape[1], 128))

    def drain(kind, count):
        def one_step(at, _):
            for one in sends(kind, at, range(4)):
                one.wait_send()
            return 0

        lax.fori_loop(0, count, one_step, 0)

    def gradients(hid, dgate, dup, next_hid, before_first, gd, ggu):
        def down(j, _):
            slot = j % 2
            load_b(hid, j, slot).wait()
            put(1, j, dot(a_buf[0], b_buf[slot]))

            @pl.when(j < steps - 2)
            def _():
                load_b(hid, j + 2, slot).start()

            @pl.when(j >= steps - 2)
            def _():
                load_b(dgate, j + 2 - steps, slot).start()

            @pl.when(j == 0)
            def _():
                before_first()

            start(sends(1, j, (0, 1)))
            return 0

        lax.fori_loop(0, steps, down, 0)
        load_a(a1, 1, 1).wait()

        def gate_up(i, _):
            slot = i % 2
            load_b(dgate, i % steps, slot).wait()
            put(0, i, dot(a_buf[1], b_buf[slot]))

            start(sends(0, i, (0, 1)))

            @pl.when(i < steps - 2)
            def _():
                load_b(dgate, i + 2, slot).start()

            @pl.when((i >= steps - 2) & (i < 2 * steps - 2))
            def _():
                load_b(dup, i + 2 - steps, slot).start()

            if next_hid is not None:

                @pl.when(i >= 2 * steps - 2)
                def _():
                    load_b(next_hid, i + 2 - 2 * steps, slot).start()

            @pl.when(i < steps)
            def _():
                pass_on(1, i)

            @pl.when(i >= steps)
            def _():
                pass_on(0, i - steps)
                finish(1, i - steps, gd, ggu)

            return 0

        lax.fori_loop(0, 2 * steps, gate_up, 0)

    load_a(dy_t, 0, 0).start()
    load_b(hid1, 0, 0).start()
    load_b(hid1, 1, 1).start()
    load_a(a1, 1, 1).start()
    barrier = pltpu.get_barrier_semaphore()
    for peer in (right, left, across):
        pl.semaphore_signal(barrier, inc=1, device_id={axis: peer}, device_id_type=mesh_id)
    total_ref[...] = jnp.zeros_like(total_ref)
    weights = [
        pltpu.make_async_copy(wg.at[1], wg_buf, w_sem.at[0]),
        pltpu.make_async_copy(wu.at[1], wu_buf, w_sem.at[1]),
        pltpu.make_async_copy(wd.at[0], wd_buf, w_sem.at[2]),
    ]

    def tile_loads(i, slot):
        at = pl.ds(pl.multiple_of(i * rows_tile, rows_tile), rows_tile)
        blocks = [(one.at[:, at], buf) for one, buf in ((dgate1, dgate_buf), (dup1, dup_buf))]
        pairs = ((act0, act_buf), (slope0, slope_buf), (h1, h_buf), (dy, dy_buf))
        blocks += [(one.at[at], buf) for one, buf in pairs]
        return [pltpu.make_async_copy(a, b.at[slot], tile_sem.at[slot, k]) for k, (a, b) in enumerate(blocks)]

    def tile_stores(i, slot):
        at = pl.ds(pl.multiple_of(i * rows_tile, rows_tile), rows_tile)
        pairs = ((dgate_out, dgate0), (dup_out, dup0))
        return [pltpu.make_async_copy(a.at[slot], b.at[:, at], out_sem.at[slot, k]) for k, (a, b) in enumerate(pairs)]

    load_a(dy_t, 0, 0).wait()
    start(weights)
    start(tile_loads(0, 0))
    gradients(hid1, dgate1, dup1, hid0, lambda: pl.semaphore_wait(barrier, 3), gd1, ggu1)

    load_a(a0, 1, 1).start()
    for one in weights:
        one.wait()
    tiles = a_buf.shape[2] // rows_tile

    def tile_back(i, _):
        slot = i % 2
        at = pl.ds(pl.multiple_of(i * rows_tile, rows_tile), rows_tile)
        for one in tile_loads(i, slot):
            one.wait()

        @pl.when(i < tiles - 1)
        def _():
            start(tile_loads(i + 1, 1 - slot))

        @pl.when(i >= 2)
        def _():
            for one in tile_stores(i - 2, slot):
                one.wait()

        da = [
            sum(dot(w[:, c * tile : (c + 1) * tile], by[slot, c], NT) for c in range(steps)).astype(BF16)
            for w, by in ((wg_buf, dgate_buf), (wu_buf, dup_buf))
        ]
        da = da[0] + da[1]
        da = da.astype(F32).T
        wide = h_buf[slot].astype(F32)
        scale = scale_of(wide)
        along = jnp.mean(da * wide, -1, keepdims=True)
        dn = da * scale - wide * (scale * scale * scale * along)
        dh = (dy_buf[slot].astype(F32) + dn.astype(BF16).astype(F32)).astype(BF16)
        a_buf[0, :, at] = dh.T
        for c in range(steps):
            to = pl.ds(c * tile, tile)
            dhid = dot(dh, wd_buf[to, :], NT).astype(BF16).astype(F32)
            dgate_out[slot, c] = (dhid * slope_buf[slot, :, to]).astype(BF16)
            dup_out[slot, c] = (dhid * act_buf[slot, :, to]).astype(BF16)
        start(tile_stores(i, slot))

        ended = tiles - 2 * steps

        @pl.when((i >= ended - steps) & (i < ended))
        def _():
            pass_on(0, i - ended + 2 * steps)

        @pl.when(i >= ended)
        def _():
            finish(0, i - ended, gd1, ggu1)

        return 0

    lax.fori_loop(0, tiles, tile_back, 0)
    for peer in (right, left):
        pl.semaphore_signal(ready, inc=1, device_id={axis: peer}, device_id_type=mesh_id)
    for i in (tiles - 2, tiles - 1):
        for one in tile_stores(i, i % 2):
            one.wait()
    drain(1, steps)
    drain(0, 2 * steps)

    gradients(hid0, dgate0, dup0, None, lambda: pl.semaphore_wait(ready, 2), gd0, ggu0)

    def rest(i, _):
        pass_on(0, steps + i)
        finish(0, i, gd0, ggu0)
        return 0

    def final(i, _):
        finish(0, steps + i, gd0, ggu0)
        return 0

    lax.fori_loop(0, steps, rest, 0)
    lax.fori_loop(0, steps, final, 0)

    norms[3] = total_ref[...]
    copies = [
        pltpu.make_async_remote_copy(
            src_ref=norms.at[3],
            dst_ref=norms.at[to],
            send_sem=norm_sem.at[0, to],
            recv_sem=norm_sem.at[1, to],
            device_id={axis: peer},
            device_id_type=mesh_id,
        )
        for to, peer in enumerate((right, left, across))
    ]
    start(copies)
    drain(1, steps)
    drain(0, 2 * steps)
    for one in copies:
        one.wait()
    total = jnp.sum((norms[0] + norms[1]) + (norms[2] + norms[3]), keepdims=True)
    factor = jnp.minimum(1.0, 0.5 * lax.rsqrt(total / (3.0 * wg.shape[0] * wg.shape[1] * wg.shape[2]) + 1e-30))
    total_ref[...] = jnp.broadcast_to(factor, total_ref.shape)


def back(dy, dy_t, a1, hid1, dgate1, dup1, h1, act0, slope0, hid0, a0, wg, wu, wd, rows_tile=256):
    t, d = dy.shape
    steps, _, tile = hid1.shape
    f = steps * tile
    shapes, counts = ((d // (2 * N), tile), (tile // (2 * N), d)), (2 * steps, steps)

    def each(*parts):
        return [pltpu.VMEM((counts[k], *parts, *shapes[k]), BF16) for k in range(2)]

    any_spec, vmem_spec = pl.BlockSpec(memory_space=pl.ANY), pl.BlockSpec(memory_space=pltpu.VMEM)
    down, gate_up = jax.ShapeDtypeStruct((f // N, d), BF16), jax.ShapeDtypeStruct((2, d // N, f), BF16)
    return pl.pallas_call(
        functools.partial(back_kernel, "dp", tile, rows_tile),
        in_specs=[any_spec] * 14,
        out_specs=[vmem_spec] * 5 + [any_spec] * 2,
        out_shape=[down, down, gate_up, gate_up, jax.ShapeDtypeStruct((8, 128), F32)] + [blocks_shape(t, f)] * 2,
        scratch_shapes=[
            pltpu.VMEM((2, d, t), BF16),
            pltpu.VMEM((2, t, tile), BF16),
            pltpu.VMEM((d, f), BF16),
            pltpu.VMEM((d, f), BF16),
            pltpu.VMEM((f, d), BF16),
            pltpu.VMEM((2, steps, rows_tile, tile), BF16),
            pltpu.VMEM((2, steps, rows_tile, tile), BF16),
            pltpu.VMEM((2, rows_tile, f), F32),
            pltpu.VMEM((2, rows_tile, f), F32),
            pltpu.VMEM((2, rows_tile, d), BF16),
            pltpu.VMEM((2, rows_tile, d), BF16),
            pltpu.VMEM((2, steps, rows_tile, tile), BF16),
            pltpu.VMEM((2, steps, rows_tile, tile), BF16),
            each(2 * N),
            each(2),
            each(2),
            each(),
            each(),
            [pltpu.VMEM((d, tile), BF16), pltpu.VMEM((tile, d), BF16)],
            pltpu.VMEM((4, 8, 128), F32),
            pltpu.SemaphoreType.DMA((2,)),
            pltpu.SemaphoreType.DMA((2,)),
            pltpu.SemaphoreType.DMA((3,)),
            pltpu.SemaphoreType.DMA((2, 6)),
            pltpu.SemaphoreType.DMA((2, 2)),
            pltpu.SemaphoreType.REGULAR,
            pltpu.SemaphoreType.DMA((2, 3)),
            pltpu.SemaphoreType.DMA((4, 3 * steps)),
            pltpu.SemaphoreType.DMA((4, 3 * steps)),
        ],
        compiler_params=pltpu.CompilerParams(vmem_limit_bytes=67_000_000, collective_id=1, has_side_effects=True),
        cost_estimate=cost(18 * t * d * f, 40 * t * f),
        name="back",
    )(dy, dy_t, a1, hid1, dgate1, dup1, h1, act0, slope0, hid0, a0, wg, wu, wd)[:5]


def adamw(w, m, v, g):
    m = 0.9 * m + 0.1 * g
    v = 0.95 * v + 0.05 * g * g
    step = m * lax.rsqrt(v + 1e-8) + 0.1 * w
    return (w - 0.02 * step).astype(BF16), m, v


def update_kernel(me_ref, factor_ref, g_ref, m_ref, v_ref, w_ref, *refs):
    new_w, new_m, new_v = refs[-3:]
    g = g_ref[...].astype(F32) * factor_ref[0:1, 0:1]
    new_w[...], new_m[...], new_v[...] = adamw(w_ref[...].astype(F32), m_ref[...], v_ref[...], g)


def update(me, factor, g, which, m, v, w, layer, into):
    rows, columns = m.shape[1:]
    size = 32 if rows < 256 else 128
    blocks = rows // size
    own = pl.BlockSpec((None, size, columns), lambda i, me: (layer, i, 0))
    if g.ndim == 3:
        g_spec = pl.BlockSpec((None, size, columns), lambda i, me: (which, i, 0))
    else:
        g_spec = pl.BlockSpec((size, columns), lambda i, me: (i, 0))
    return pl.pallas_call(
        update_kernel,
        grid_spec=pltpu.PrefetchScalarGridSpec(
            num_scalar_prefetch=1,
            grid=(blocks,),
            in_specs=[
                pl.BlockSpec((8, 128), lambda i, me: (0, 0)),
                g_spec,
                own,
                own,
                pl.BlockSpec((None, size, columns), lambda i, me: (layer, me[0] * blocks + i, 0)),
            ]
            + [pl.BlockSpec(memory_space=pl.ANY)] * len(into),
            out_specs=[pl.BlockSpec((size, columns), lambda i, me: (i, 0)), own, own],
        ),
        out_shape=[jax.ShapeDtypeStruct((rows, columns), BF16)] + [jax.ShapeDtypeStruct(m.shape, F32)] * 2,
        input_output_aliases={6 + k: 1 + k for k in range(len(into))},
        compiler_params=params(),
        cost_estimate=cost(2_000_000_000, 22 * rows * columns),
    )(me, factor, g, m, v, w, *into)


def place_kernel(axis, where, *refs):
    blocks, refs = refs[: len(where)], refs[len(where) :]
    outs, sems = refs[-4:-1], refs[-1]
    me = lax.axis_index(axis)
    copies = []
    for k, (matrix, layer, shift, start) in enumerate(where):
        rows = outs[matrix].shape[1] // 4
        at = ((me + shift) % 4) * rows + start
        size = blocks[k].shape[0]
        copies.append(pltpu.make_async_copy(blocks[k], outs[matrix].at[layer, pl.ds(pl.multiple_of(at, 16), size), :], sems.at[k]))
    for one in copies:
        one.start()
    for one in copies:
        one.wait()


def place(blocks, where, shapes, into):
    any_spec, vmem_spec = pl.BlockSpec(memory_space=pl.ANY), pl.BlockSpec(memory_space=pltpu.VMEM)
    into = list(into)
    return pl.pallas_call(
        functools.partial(place_kernel, "dp", where),
        in_specs=[vmem_spec] * len(blocks) + [any_spec] * len(into),
        out_specs=[any_spec] * 3,
        out_shape=[jax.ShapeDtypeStruct(s, BF16) for s in shapes],
        scratch_shapes=[pltpu.SemaphoreType.DMA((len(blocks),))],
        input_output_aliases={len(blocks) + k: k for k in range(len(into))},
        compiler_params=params(),
        cost_estimate=cost(1000, sum(b.size for b in blocks) * 4),
    )(*blocks, *into)


def solution(mesh):
    n = mesh.shape["dp"]
    to_right = [(i, (i + 1) % n) for i in range(n)]
    to_left = [(i, (i - 1) % n) for i in range(n)]

    def body(x, dy, wg, wu, wd, *moments):
        m, v = moments[:3], moments[3:]
        x, dy = x[0], dy[0]
        act0, slope0, hid0, h1, a0, hid1, dgate1, dup1, a1, dy_t = front(x, dy, wg, wu, wd)
        gd0, gd1, ggu0, ggu1, factor = back(dy, dy_t, a1, hid1, dgate1, dup1, h1, act0, slope0, hid0, a0, wg, wu, wd)
        me = lax.axis_index("dp").astype(jnp.int32).reshape(1)
        weights = (wg, wu, wd)
        new, blocks, where, direct = [(), (), ()], [], [], {}
        for k in range(3):
            for layer, g in enumerate((gd0, gd1) if k == 2 else (ggu0, ggu1)):
                own, *new[k] = update(me, factor, g, k, m[k], v[k], weights[k], layer, new[k])
                from_left = lax.ppermute(own, "dp", to_right)
                from_right = lax.ppermute(own, "dp", to_left)
                direct[k, layer] = (from_left, from_right)
                blocks += [own, from_left, from_right]
                where += [(k, layer, 0, 0), (k, layer, n - 1, 0), (k, layer, 1, 0)]
        shapes = [w.shape for w in weights]
        whole = place(blocks, where, shapes, ())
        far = []
        for (k, layer), (from_left, from_right) in direct.items():
            half = from_left.shape[0] // 2
            far += [
                (lax.ppermute(from_left[:half], "dp", to_right), (k, layer, 2, 0)),
                (lax.ppermute(from_right[half:], "dp", to_left), (k, layer, 2, half)),
            ]
        for part in (far[:10], far[10:]):
            whole = place([one[0] for one in part], [one[1] for one in part], shapes, whole)
        return (*whole, *(one[0] for one in new), *(one[1] for one in new))

    whole, rows = P(None, None, None), P(None, "dp", None)
    return jax.shard_map(
        body,
        mesh=mesh,
        in_specs=(P(("rep", "dp")),) * 2 + (whole,) * 3 + (rows,) * 6,
        out_specs=(P("rep"),) * 3 + (P("rep", "dp"),) * 6,
        check_vma=False,
    )
```
